32 devices in a mesh: groups: 2 (over y), ctx: 4 (over z), tp: 4 (over x, core).
Axes of the slice: x: 2, y: 2, z: 4, core: 2. Of those that a mesh axis runs over, the one named last changes fastest.
Arguments:
- query_matrix: bfloat16 [1024, 8192], P(('groups', 'ctx'), 'tp'), parts along dimension 0, may hold values from -20 to 20
- key_matrix: bfloat16 [1024, 1024], P(('groups', 'ctx'), 'tp'), parts along dimension 0, may hold values from -20 to 20
- value_matrix: bfloat16 [1024, 1024], P(('groups', 'ctx'), 'tp'), parts along dimension 0, may hold values from -6 to 6
- doc_ids: int32 [1024], P('groups'), parts along dimension 0, may hold values from 0 to 5, never falling along the last dimension, each value on 1 to 256 neighbouring positions
- out_weight: bfloat16 [8192, 4096], P('tp', 'ctx'), may hold values from -0.0625 to 0.0625
Outputs:
- projected: bfloat16 [1024, 4096], P(('groups', 'ctx'), 'tp'), parts along dimension 0
The draws below stay inside these ranges and needn't reach their ends.
There are 2 independent parts, one for each index of `groups`. The reference program is written for one: setup_inputs(seed, part) draws one part's arguments, and reference() takes and returns one part's arrays. A program takes and returns all parts, laid end to end along the dimension named above; an argument that names none is the same for every part. Nothing has to cross between parts.
Inputs may be any that keep to these rules, and one draw needn't show every extreme that they name: `doc_ids`: non-decreasing along the sequence; each document holds 1 to 256 tokens, one exactly 256.
All inputs are finite; a program needn't handle non-finite values.
Results may differ from the reference program's by a relative error of at most 0.015.
Values may be sent and summed in bfloat16 or wider, within the bound.
A program may use at most 64 MiB of HBM per device.

```python
import math
import jax
import jax.numpy as jnp
import numpy as np
from jax import lax

QUERY_HEAD_COUNT = 64
KEY_VALUE_HEADS = 8
HEAD_SIZE = 128
DWIN = 4096
DOCS = 6
SEQUENCE_TOKENS = 512
N_TP = 4


def draw_query_matrix(key, part):
    column_list = QUERY_HEAD_COUNT * HEAD_SIZE
    noise_key = jax.random.fold_in(key, 101)
    values = jnp.clip(1.7 * jax.random.normal(noise_key, (SEQUENCE_TOKENS, column_list)), -7.0, 7.0)
    return values.astype(jnp.bfloat16)


def draw_key_matrix(key, part):
    column_list = KEY_VALUE_HEADS * HEAD_SIZE
    noise_key = jax.random.fold_in(key, 202)
    values = jnp.clip(1.7 * jax.random.normal(noise_key, (SEQUENCE_TOKENS, column_list)), -7.0, 7.0)
    return values.astype(jnp.bfloat16)


def block_levels(key, extent, cuts, least, high):
    loudness = 1.0
    for position, shards_of in cuts:
        steps = jax.random.uniform(jax.random.fold_in(jax.random.fold_in(key, 6), position), (shards_of,), jnp.float32, least / len(cuts), high / len(cuts))
        loudness = loudness * jnp.repeat(jnp.exp(steps), extent[position] // shards_of).reshape((-1,) + (1,) * (len(extent) - 1 - position))
    return loudness


def split_up(count, total, limit, slope):
    portions = [(1 << 20) // math.isqrt(rank ** slope) + 1 for rank in range(2, count + 1)]
    surplus, holding = total - limit - (count - 1), [1] * (count - 1)
    while surplus > 0:
        free = [i for i in range(count - 1) if holding[i] < limit]
        mass, remaining = sum([portions[i] for i in free]), surplus
        for i in free:
            addition = min(limit - holding[i], max(1, remaining * portions[i] // mass), surplus)
            holding[i] = holding[i] + addition
            surplus = surplus - addition
    return np.array([limit] + holding)


def ragged_sizes(own_key, count, total, bound, lean):
    if count == 2:
        one = jax.random.randint(own_key, (), max(1, total - bound), min(bound, total - 1) + 1)
        return jnp.stack([one, total - one])
    lengths = jnp.asarray(split_up(count, total, bound, lean), jnp.int32)
    pairs = (count - 1) // 2
    giver, taker = lengths[1:1 + 2 * pairs:2], lengths[2:2 + 2 * pairs:2]
    slack = jnp.minimum(giver - 1, bound - taker)
    moved = jax.random.randint(jax.random.fold_in(own_key, 1), (pairs,), 0, 1 << 20) % (slack + 1)
    lengths = lengths.at[1:1 + 2 * pairs:2].set(giver - moved).at[2:2 + 2 * pairs:2].set(taker + moved)
    return lengths[jax.random.permutation(jax.random.fold_in(own_key, 2), count)]


def normal_values(stream_key, extent, spread, reach, cuts=(), held_as=jnp.bfloat16):
    values = spread * jax.random.normal(stream_key, extent, jnp.float32)
    if cuts:
        values = values * block_levels(stream_key, extent, cuts, -0.22, 0.18)
    return jnp.clip(values, -reach, reach).astype(held_as)


def setup_inputs(seed: int = 0, part: int = 0) -> dict:
    streams_of = jax.random.split(jax.random.key(seed), 6)
    own_keys = jax.random.split(jax.random.fold_in(streams_of[5], part), 6)
    query_matrix = draw_query_matrix(jax.random.fold_in(jax.random.fold_in(streams_of[5], part), 71), part)
    key_matrix = draw_key_matrix(jax.random.fold_in(jax.random.fold_in(streams_of[5], part), 71), part)
    value_matrix = normal_values(own_keys[2], (SEQUENCE_TOKENS, KEY_VALUE_HEADS * HEAD_SIZE), 1.0, 6.0, ((0, 4), (1, 4)))
    doc_ids = jnp.searchsorted(jnp.cumsum(ragged_sizes(own_keys[3], DOCS, SEQUENCE_TOKENS, SEQUENCE_TOKENS // 2, 0)), jnp.arange(SEQUENCE_TOKENS), side="right").astype(jnp.int32)
    out_weight = normal_values(streams_of[4], (QUERY_HEAD_COUNT * HEAD_SIZE, DWIN), (QUERY_HEAD_COUNT * HEAD_SIZE) ** -0.5, 0.0625, ((0, 4), (1, 4)))
    return dict(query_matrix=query_matrix, key_matrix=key_matrix, value_matrix=value_matrix, doc_ids=doc_ids, out_weight=out_weight)


rope_base = 1000000.0


def rotary_tables(rows, token_positions, heads):
    half_dim = HEAD_SIZE // 2
    frequency = jnp.power(jnp.float32(rope_base), -jnp.arange(half_dim, dtype=jnp.float32) * (2.0 / HEAD_SIZE))
    angles = token_positions.astype(jnp.float32)[:, None] * frequency[None, :]
    cosine = jnp.cos(angles)[:, None, :]
    sine = jnp.sin(angles)[:, None, :]
    values = rows.astype(jnp.float32).reshape(rows.shape[0], heads, HEAD_SIZE)
    first = values[..., :half_dim]
    second = values[..., half_dim:]
    turned = jnp.concatenate([first * cosine - second * sine, second * cosine + first * sine], -1)
    return turned.reshape(rows.shape[0], heads * HEAD_SIZE).astype(jnp.bfloat16)


def reference(query_matrix, key_matrix, value_matrix, doc_ids, out_weight):
    group_width = QUERY_HEAD_COUNT // KEY_VALUE_HEADS
    inverse_root = HEAD_SIZE ** -0.5
    token_positions = jnp.arange(SEQUENCE_TOKENS, dtype=jnp.int32)
    query_matrix_rot = rotary_tables(query_matrix, token_positions, QUERY_HEAD_COUNT).astype(jnp.float32).reshape(SEQUENCE_TOKENS, KEY_VALUE_HEADS, group_width, HEAD_SIZE).transpose(1, 0, 2, 3)
    every_key = rotary_tables(key_matrix, token_positions, KEY_VALUE_HEADS).astype(jnp.float32).reshape(SEQUENCE_TOKENS, KEY_VALUE_HEADS, HEAD_SIZE).transpose(1, 0, 2)
    every_value = value_matrix.astype(jnp.float32).reshape(SEQUENCE_TOKENS, KEY_VALUE_HEADS, HEAD_SIZE).transpose(1, 0, 2)
    block_rows = math.gcd(SEQUENCE_TOKENS, 512)
    block_count = SEQUENCE_TOKENS // block_rows

    def one_head(inputs):
        head_q, head_k, head_v = inputs

        def one_block(block_index):
            first_row = block_index * block_rows
            block_q = lax.dynamic_slice_in_dim(head_q, first_row, block_rows, 0)
            query_pos = first_row + jnp.arange(block_rows, dtype=jnp.int32)
            query_doc = lax.dynamic_slice_in_dim(doc_ids, first_row, block_rows, 0)
            scores = jnp.einsum("qgd,sd->gqs", block_q, head_k) * inverse_root
            allowed = ((query_doc[:, None] == doc_ids[None, :]) & (token_positions[None, :] <= query_pos[:, None]))[None]
            row_max = jnp.max(jnp.where(allowed, scores, -1e30), axis=-1, keepdims=True)
            weights = jnp.where(allowed, jnp.exp(scores - row_max), 0.0)
            totals = jnp.sum(weights, -1)
            rounded = lax.optimization_barrier(weights.astype(jnp.bfloat16)).astype(jnp.float32)
            mixed_rows = jnp.einsum("gqs,sd->qgd", rounded, head_v)
            return mixed_rows / totals.T[:, :, None]

        return lax.map(one_block, jnp.arange(block_count, dtype=jnp.int32)).reshape(SEQUENCE_TOKENS, group_width, HEAD_SIZE)

    attended = lax.map(one_head, (query_matrix_rot, every_key, every_value))
    attention = attended.transpose(1, 0, 2, 3).reshape(SEQUENCE_TOKENS, QUERY_HEAD_COUNT * HEAD_SIZE).astype(jnp.bfloat16)
    share_rows = QUERY_HEAD_COUNT * HEAD_SIZE // N_TP
    projected = jnp.zeros((SEQUENCE_TOKENS, DWIN), jnp.float32)
    for member in range(N_TP):
        partial_sum = jnp.dot(attention[:, member * share_rows:(member + 1) * share_rows],
                              out_weight[member * share_rows:(member + 1) * share_rows],
                              preferred_element_type=jnp.float32)
        projected = projected + lax.optimization_barrier(partial_sum.astype(jnp.bfloat16)).astype(jnp.float32)
    return projected.astype(jnp.bfloat16)
```

```python
import functools
import math

import jax
import jax.numpy as jnp
import numpy as np
from jax import lax
from jax.experimental import pallas as pl
from jax.experimental.pallas import tpu as pltpu
from jax.sharding import PartitionSpec as P

MESH = pl.DeviceIdType.MESH

HEAD_SIZE = 128


rope_base = 1000000.0


def rotary_tables(rows, token_positions, heads):
    half_dim = HEAD_SIZE // 2
    frequency = jnp.power(
        jnp.float32(rope_base), -jnp.arange(half_dim, dtype=jnp.float32) * (2.0 / HEAD_SIZE)
    )
    angles = token_positions.astype(jnp.float32)[:, None] * frequency[None, :]
    cosine = jnp.cos(angles)[:, None, :]
    sine = jnp.sin(angles)[:, None, :]
    values = rows.astype(jnp.float32).reshape(rows.shape[0], heads, HEAD_SIZE)
    first = values[..., :half_dim]
    second = values[..., half_dim:]
    turned = jnp.concatenate([first * cosine - second * sine, second * cosine + first * sine], -1)
    return turned.reshape(rows.shape[0], heads * HEAD_SIZE).astype(jnp.bfloat16)


def on_device(query_matrix, key_matrix, value_matrix, doc_ids, out_weight):
    ctx_index = lax.axis_index("ctx")
    tok_rows = query_matrix.shape[0]
    query_heads = query_matrix.shape[1] // HEAD_SIZE
    key_heads = key_matrix.shape[1] // HEAD_SIZE
    group_width = query_heads // key_heads
    inverse_root = HEAD_SIZE ** (-0.5)
    local_rows = jnp.arange(tok_rows, dtype=jnp.int32)
    given_pos = ctx_index * tok_rows + local_rows
    query_matrix_rot = rotary_tables(query_matrix, given_pos, query_heads)
    keys_here = rotary_tables(key_matrix, given_pos, key_heads)
    query_doc = jnp.take(doc_ids, given_pos, axis=0)
    query_four = query_matrix_rot.reshape(tok_rows, key_heads, group_width, HEAD_SIZE)

    def attend(state, block):
        key_block, value_block, doc_block, pos_block = block
        row_max, totals, accum = state
        scores = (
            jnp.einsum("qkgd,skd->kgqs", query_four, key_block, preferred_element_type=jnp.float32)
            * inverse_root
        )
        allowed = (
            (query_doc[:, None] == doc_block[None, :]) & (pos_block[None, :] <= given_pos[:, None])
        )[None, None]
        new_max = jnp.maximum(row_max, jnp.max(jnp.where(allowed, scores, -1e30), -1))
        weights = jnp.where(allowed, jnp.exp(scores - new_max[..., None]), 0.0)
        factor = jnp.exp(row_max - new_max)
        totals = totals * factor + jnp.sum(weights, -1)
        accum = accum * jnp.transpose(factor, (2, 0, 1))[..., None] + jnp.einsum(
            "kgqs,skd->qkgd",
            weights.astype(jnp.bfloat16),
            value_block,
            preferred_element_type=jnp.float32,
        )
        return (new_max, totals, accum)

    start_state = (
        jnp.full((key_heads, group_width, tok_rows), -1e30, jnp.float32),
        jnp.zeros((key_heads, group_width, tok_rows), jnp.float32),
        jnp.zeros((tok_rows, key_heads, group_width, HEAD_SIZE), jnp.float32),
    )
    key_piece = lax.all_gather(keys_here, "ctx", axis=0, tiled=True)
    value_piece = lax.all_gather(value_matrix, "ctx", axis=0, tiled=True)
    count = key_piece.shape[0]
    block_rows = math.gcd(count, 512)
    block_count = count // block_rows
    positions = jnp.arange(count, dtype=jnp.int32)
    blocks = (
        key_piece.reshape(block_count, block_rows, key_heads, HEAD_SIZE),
        value_piece.reshape(block_count, block_rows, key_heads, HEAD_SIZE),
        jnp.take(doc_ids, positions, axis=0).reshape(block_count, block_rows),
        positions.reshape(block_count, block_rows),
    )

    def step_block(inner_state, block):
        return (attend(inner_state, block), None)

    final_state, unused_out = lax.scan(step_block, start_state, blocks)
    row_max, totals, accum = final_state
    attention = (
        (accum / jnp.transpose(totals, (2, 0, 1))[..., None])
        .reshape(tok_rows, query_heads * HEAD_SIZE)
        .astype(jnp.bfloat16)
    )
    terms = jnp.dot(
        attention,
        lax.all_gather(out_weight, "ctx", axis=1, tiled=True),
        preferred_element_type=jnp.float32,
    )
    return lax.psum_scatter(terms.astype(jnp.bfloat16), "tp", scatter_dimension=1, tiled=True)


def fused_kernel(
    n, groups, back, query_ref, key_ref, value_ref, doc_ref, table_ref, weight_ref, out_ref,
    query_in, key_in, table, docs, weight, lent, rotated, bias, kv, gathered, total_lo, total_hi,
    partial, pair_in, crossing, cross_in, summed, landed, landed_aid,
    load_sem, weight_sem, kv_send, kv_recv, up_send, down_send, chunk_recv, lend_send, lend_recv,
    share_send, share_recv, pair_send, pair_recv, cross_send, cross_recv, result_send, result_recv, aid_recv, store_sem,
):
    group = lax.axis_index("groups")
    ctx = lax.axis_index("ctx")
    tp = lax.axis_index("tp")
    rows = query_ref.shape[0]
    kv_heads = key_ref.shape[1] // HEAD_SIZE
    query_heads = query_ref.shape[1] // HEAD_SIZE
    group_width = query_heads // kv_heads
    chunks = gathered.shape[1]
    chunk_width = gathered.shape[3]
    chunk_heads = chunk_width // HEAD_SIZE
    quarter = partial.shape[3]
    last = n - 1
    lent_chunk = chunks - 1
    pieces = lend_send.shape[0]
    half_rows = chunk_width // groups
    piece_rows = half_rows // pieces
    is_edge = (ctx == 0) | (ctx == last)
    is_helper = (ctx == 1) | (ctx == last - 1)
    helped = jnp.where(ctx == 1, 0, last)
    other_group = lax.rem(group + 1, groups)
    pair = tp + 1 - 2 * lax.rem(tp, 2)
    across = lax.rem(tp + 2, n)
    pair_across = lax.rem(pair + 2, n)

    def remote(src, dst, send, recv, to_ctx, to_tp):
        return pltpu.make_async_remote_copy(
            src_ref=src, dst_ref=dst, send_sem=send, recv_sem=recv,
            device_id={"ctx": to_ctx, "tp": to_tp}, device_id_type=MESH,
        )

    barrier = pltpu.get_barrier_semaphore()

    def greet(**device):
        pl.semaphore_signal(barrier, inc=1, device_id=device, device_id_type=MESH)

    @pl.when(ctx > 0)
    def _():
        greet(ctx=ctx - 1)

    @pl.when(ctx < last)
    def _():
        greet(ctx=ctx + 1)

    @pl.when(ctx == back)
    def _():
        greet(ctx=ctx - back)

    for step in range(1, n):
        greet(tp=lax.rem(tp + step, n))

    @pl.when(is_helper)
    def _():
        greet(groups=other_group)

    greetings = n - 1 + sum(
        flag.astype(jnp.int32) for flag in (ctx > 0, ctx < last, ctx == 0, is_helper)
    )

    first_row = pl.multiple_of(ctx * rows, rows)
    loads = [
        pltpu.make_async_copy(key_ref, key_in, load_sem.at[0]),
        pltpu.make_async_copy(table_ref.at[:, pl.ds(first_row, rows)], table, load_sem.at[1]),
        pltpu.make_async_copy(doc_ref, docs, load_sem.at[2]),
        pltpu.make_async_copy(query_ref, query_in, load_sem.at[3]),
    ]
    value_loads = [
        pltpu.make_async_copy(
            value_ref.at[:, pl.ds(head * HEAD_SIZE, HEAD_SIZE)], kv.at[back, head, 1], load_sem.at[4 + head]
        )
        for head in range(kv_heads)
    ]
    weight_loads = [
        pltpu.make_async_copy(
            weight_ref.at[pl.ds(chunk * chunk_width, chunk_width)], weight.at[chunk], weight_sem.at[chunk]
        )
        for chunk in [lent_chunk] + list(range(lent_chunk))
    ]
    for load in loads + value_loads + weight_loads:
        load.start()

    def turn(values):
        values = values.astype(jnp.float32)
        return (values * table[0] + pltpu.roll(values, HEAD_SIZE // 2, 1) * table[1]).astype(jnp.bfloat16)

    loads[0].wait()
    loads[1].wait()
    for head in range(kv_heads):
        kv[back, head, 0] = turn(key_in[:, head * HEAD_SIZE : (head + 1) * HEAD_SIZE])
    for load in value_loads:
        load.wait()

    for slot in range(back):
        @pl.when(ctx < back - slot)
        def _():
            kv[slot] = jnp.zeros(kv.shape[1:], kv.dtype)

    pl.semaphore_wait(barrier, greetings)

    def kv_copy(slot, head):
        return remote(
            kv.at[slot, head], kv.at[slot - 1, head], kv_send.at[slot, head], kv_recv.at[slot - 1, head],
            lax.rem(ctx + 1, n), tp,
        )

    def kv_direct(head):
        return remote(
            kv.at[back, head], kv.at[0, head], kv_send.at[0, head], kv_recv.at[0, head], lax.rem(ctx + back, n), tp
        )

    for head in range(kv_heads):
        @pl.when(ctx < last)
        def _():
            kv_copy(back, head).start()

        @pl.when(ctx == 0)
        def _():
            kv_direct(head).start()

    loads[2].wait()
    own_docs = jnp.broadcast_to(docs[pl.ds(ctx, 1), :], (rows, rows)).astype(jnp.float32).T
    row_index = lax.broadcasted_iota(jnp.int32, (rows, rows), 0)
    column_index = lax.broadcasted_iota(jnp.int32, (rows, rows), 1)
    for slot in range(back + 1):
        block = ctx - back + slot
        their_docs = docs[pl.ds(lax.max(block, 0), 1), :].astype(jnp.float32)
        allowed = (own_docs == their_docs) & (block * rows + column_index <= ctx * rows + row_index) & (block >= 0)
        bias[slot] = jnp.where(allowed, 0.0, -1e30)

    loads[3].wait()
    for head in range(query_heads):
        rotated[head] = turn(query_in[:, head * HEAD_SIZE : (head + 1) * HEAD_SIZE])

    weight_loads[0].wait()
    forwards = (ctx >= back) & (ctx < last)

    def take_kv(head):
        kv_copy(back, head).wait_recv()

        @pl.when(forwards)
        def _():
            kv_copy(back - 1, head).start()

    for head in range(kv_heads):
        @pl.when(ctx >= (1 if head == 0 else back))
        def _():
            take_kv(head)

    def lend_copy(piece):
        start = pl.multiple_of(group * half_rows + piece * piece_rows, piece_rows)
        return remote(
            weight.at[lent_chunk, pl.ds(start, piece_rows)], lent.at[pl.ds(start, piece_rows)],
            lend_send.at[piece], lend_recv.at[piece], jnp.where(ctx == 0, 1, last - 1), tp,
        )

    def share_copy(piece, owner):
        start = pl.multiple_of(owner * half_rows + piece * piece_rows, piece_rows)
        here = lent.at[pl.ds(start, piece_rows)]
        return pltpu.make_async_remote_copy(
            src_ref=here, dst_ref=here, send_sem=share_send.at[piece], recv_sem=share_recv.at[piece],
            device_id={"groups": other_group}, device_id_type=MESH,
        )

    def up_copy(block, chunk):
        here = gathered.at[block, chunk]
        return remote(here, here, up_send.at[block, chunk], chunk_recv.at[block, chunk], lax.rem(ctx + 1, n), tp)

    def down_copy(block, chunk):
        here = gathered.at[block, chunk]
        return remote(here, here, down_send.at[block, chunk], chunk_recv.at[block, chunk], lax.rem(ctx + last, n), tp)

    def goes_up(chunk):
        return ctx < (last - 1 if chunk == lent_chunk else last)

    def goes_down(chunk):
        return ctx > (1 if chunk == lent_chunk else 0)

    scale = HEAD_SIZE ** (-0.5) * math.log2(math.e)
    contract = (((1,), (1,)), ((), ()))
    for head in range(query_heads):
        kv_head = head // group_width
        if head % group_width == 0:
            if kv_head > 0:
                @pl.when((ctx >= 1) & (ctx < back))
                def _():
                    take_kv(kv_head)

            @pl.when(ctx >= back)
            def _():
                kv_copy(1, kv_head).wait_recv()

        scores = [
            lax.dot_general(rotated[head], kv[slot, kv_head, 0], contract, preferred_element_type=jnp.float32) * scale
            + bias[slot]
            for slot in range(back + 1)
        ]
        row_max = functools.reduce(jnp.maximum, scores).max(-1, keepdims=True)
        weights = [jnp.exp2(score - row_max) for score in scores]
        totals = sum(weights).sum(-1, keepdims=True)
        mixed = sum(
            jnp.dot(weights[slot].astype(jnp.bfloat16), kv[slot, kv_head, 1], preferred_element_type=jnp.float32)
            for slot in range(back + 1)
        )
        chunk, place = head // chunk_heads, head % chunk_heads
        gathered[ctx, chunk, :, place * HEAD_SIZE : (place + 1) * HEAD_SIZE] = (mixed / totals).astype(jnp.bfloat16)
        if place == chunk_heads - 1:
            @pl.when(goes_up(chunk))
            def _():
                up_copy(ctx, chunk).start()

            @pl.when(goes_down(chunk))
            def _():
                down_copy(ctx, chunk).start()

    @pl.when(is_edge)
    def _():
        for piece in range(pieces):
            lend_copy(piece).start()

    def pair_copy(place, index):
        return remote(
            partial.at[place, pair_across if index else pair], pair_in.at[place, index],
            pair_send.at[place, index], pair_recv.at[place, index], ctx, pair,
        )

    def cross_copy(place):
        return remote(
            crossing.at[place], cross_in.at[place], cross_send.at[place], cross_recv.at[place], ctx, across
        )

    parts = (pair_across, pair, across, tp)

    def part_columns(part):
        return pl.ds(pl.multiple_of(part * quarter, quarter), quarter)

    def emit(place, index, product):
        partial[place, parts[index]] = product.astype(jnp.bfloat16)
        if index < 2:
            pair_copy(place, 1 - index).start()

    def project(block, chunk, total, own):
        for index, part in enumerate(parts):
            product = jnp.dot(
                gathered[block, chunk], weight[chunk, :, part_columns(part)], preferred_element_type=jnp.float32
            )
            if chunk > 0:
                product = product + total[index]
            if chunk == lent_chunk:
                emit(block, index, product)
            elif chunk == lent_chunk - 1 and not own:
                @pl.when(is_edge)
                def _():
                    emit(block, index, product)

                @pl.when(jnp.logical_not(is_edge))
                def _():
                    total[index] = product
            else:
                total[index] = product

    def cross(place):
        pair_copy(place, 1).wait_recv()
        value = partial[place, across].astype(jnp.float32) + pair_in[place, 1].astype(jnp.float32)
        crossing[place] = value.astype(jnp.bfloat16)
        cross_copy(place).start()

    def collect(place):
        pair_copy(place, 0).wait_recv()
        value = partial[place, tp].astype(jnp.float32) + pair_in[place, 0].astype(jnp.float32)
        cross_copy(place).wait_recv()
        return (value + cross_in[place].astype(jnp.float32)).astype(jnp.bfloat16)

    def result_copy(block):
        return remote(
            summed.at[block], landed.at[tp], result_send.at[block], result_recv.at[tp], block, ctx
        )

    def finish(block):
        value = collect(block)
        mine = (block == ctx) & (tp == ctx)

        @pl.when(mine)
        def _():
            landed[tp] = value

        @pl.when(jnp.logical_not(mine))
        def _():
            summed[block] = value
            result_copy(block).start()

    for load in weight_loads[1:]:
        load.wait()
    for chunk in range(chunks):
        project(ctx, chunk, total_lo, True)

    def both_sides(step, act):
        @pl.when(ctx - step >= 0)
        def _():
            act(lax.max(ctx - step, 0))

        @pl.when((ctx + step <= last) & (step > 0))
        def _():
            act(lax.min(ctx + step, last))

    def pass_on(piece):
        lend_copy(piece).wait_recv()
        share_copy(piece, group).start()

    def aided(index):
        return jnp.where(ctx == 1, ctx + index, ctx - index)

    def aid_copy(index):
        return remote(
            summed.at[n + index], landed_aid.at[tp], result_send.at[n + index], aid_recv.at[tp],
            aided(index), helped,
        )

    def aid():
        for piece in range(pieces):
            share_copy(piece, other_group).wait_recv()
        for place in range(n - 1):
            for index, part in enumerate(parts):
                product = jnp.dot(
                    gathered[aided(place), lent_chunk], lent[:, part_columns(part)],
                    preferred_element_type=jnp.float32,
                )
                emit(n + place, index, product)
            if place:
                cross(n + place - 1)
        cross(2 * n - 2)

    def send_aid():
        for index in range(n - 1):
            value = collect(n + index)
            if index == 0:
                @pl.when(tp == helped)
                def _():
                    landed_aid[tp] = value

                @pl.when(tp != helped)
                def _():
                    summed[n] = value
                    aid_copy(0).start()
            else:
                summed[n + index] = value
                aid_copy(index).start()

    def gather_step(step, carry):
        low, high = lax.max(ctx - step, 0), lax.min(ctx + step, last)
        for chunk in range(chunks):
            has_low, has_high = ctx - step >= 0, ctx + step <= last
            if chunk == lent_chunk:
                has_low, has_high = has_low & (ctx < last), has_high & (ctx > 0)

            @pl.when(has_low)
            def _():
                up_copy(low, chunk).wait_recv()

                @pl.when(goes_up(chunk))
                def _():
                    up_copy(low, chunk).start()

            @pl.when(has_high)
            def _():
                down_copy(high, chunk).wait_recv()

                @pl.when(goes_down(chunk))
                def _():
                    down_copy(high, chunk).start()

            @pl.when(has_low)
            def _():
                project(low, chunk, total_lo, False)

            @pl.when(has_high)
            def _():
                project(high, chunk, total_hi, False)

            @pl.when(is_helper & (step == 2))
            def _():
                pass_on(chunk)

            if chunk == 0:
                both_sides(step - 1, cross)

        @pl.when(is_helper & (step == last))
        def _():
            aid()

        both_sides(step - 1, finish)
        return carry

    lax.fori_loop(1, n, gather_step, 0)
    both_sides(last, cross)

    @pl.when(is_helper)
    def _():
        send_aid()

    both_sides(last, finish)

    gets_aid = ((tp == 0) | (tp == last)) & (ctx != tp)
    aid_here = is_helper & (tp == helped)
    for part in range(n):
        @pl.when(jnp.logical_not((tp == ctx) & (tp == part)))
        def _():
            remote(
                summed.at[0], landed.at[part], result_send.at[0], result_recv.at[part], ctx, part
            ).wait_recv()

        @pl.when(gets_aid)
        def _():
            @pl.when(jnp.logical_not(aid_here & (tp == part)))
            def _():
                remote(
                    summed.at[n], landed_aid.at[part], result_send.at[n], aid_recv.at[part], ctx, part
                ).wait_recv()

            whole = landed[part].astype(jnp.float32) + landed_aid[part].astype(jnp.float32)
            landed[part] = whole.astype(jnp.bfloat16)

        pltpu.make_async_copy(
            landed.at[part], out_ref.at[:, pl.ds(part * quarter, quarter)], store_sem.at[part]
        ).start()

    for head in range(kv_heads):
        @pl.when(ctx < last)
        def _():
            kv_copy(back, head).wait_send()

        @pl.when(ctx == 0)
        def _():
            kv_direct(head).wait_send()

        @pl.when(forwards)
        def _():
            kv_copy(back - 1, head).wait_send()

    for piece in range(pieces):
        @pl.when(is_edge)
        def _():
            lend_copy(piece).wait_send()

        @pl.when(is_helper)
        def _():
            share_copy(piece, group).wait_send()

    def drain(block, carry):
        for chunk in range(chunks):
            @pl.when((block <= ctx) & goes_up(chunk))
            def _():
                up_copy(block, chunk).wait_send()

            @pl.when((block >= ctx) & goes_down(chunk))
            def _():
                down_copy(block, chunk).wait_send()

        for index in range(2):
            pair_copy(block, index).wait_send()
        cross_copy(block).wait_send()

        @pl.when(jnp.logical_not((block == ctx) & (tp == ctx)))
        def _():
            result_copy(block).wait_send()

        return carry

    lax.fori_loop(0, n, drain, 0)

    @pl.when(is_helper)
    def _():
        for index in range(n - 1):
            for side in range(2):
                pair_copy(n + index, side).wait_send()
            cross_copy(n + index).wait_send()
            if index == 0:
                @pl.when(tp != helped)
                def _():
                    aid_copy(0).wait_send()
            else:
                aid_copy(index).wait_send()

    for part in range(n):
        pltpu.make_async_copy(
            landed.at[part], out_ref.at[:, pl.ds(part * quarter, quarter)], store_sem.at[part]
        ).wait()


def key_blocks_back(tokens, rows):
    return -(-(tokens // 2 - 1) // rows)


def fused(n, groups, query_matrix, key_matrix, value_matrix, doc_ids, out_weight):
    rows, query_width = query_matrix.shape
    query_heads, kv_heads = query_width // HEAD_SIZE, key_matrix.shape[1] // HEAD_SIZE
    features = out_weight.shape[1]
    tokens = doc_ids.shape[0]
    back = key_blocks_back(tokens, rows)
    chunks = 4
    chunk_width = query_width // chunks
    quarter = features // n
    half = HEAD_SIZE // 2
    frequency = np.power(np.float32(rope_base), -np.arange(half, dtype=np.float32) * np.float32(2.0 / HEAD_SIZE))
    angles = np.arange(tokens, dtype=np.float32)[:, None] * frequency[None, :]
    cosine, sine = np.cos(angles), np.sin(angles)
    table = np.stack([np.concatenate([cosine, cosine], 1), np.concatenate([-sine, sine], 1)]).astype(np.float32)
    any_space = pl.BlockSpec(memory_space=pl.ANY)
    bf16, f32, dma = jnp.bfloat16, jnp.float32, pltpu.SemaphoreType.DMA
    return pl.pallas_call(
        functools.partial(fused_kernel, n, groups, back),
        out_shape=jax.ShapeDtypeStruct((rows, features), bf16),
        in_specs=[any_space] * 6,
        out_specs=any_space,
        scratch_shapes=[
            pltpu.VMEM((rows, query_width), bf16),
            pltpu.VMEM((rows, kv_heads * HEAD_SIZE), bf16),
            pltpu.VMEM((2, rows, HEAD_SIZE), f32),
            pltpu.VMEM((tokens // rows, rows), jnp.int32),
            pltpu.VMEM((chunks, chunk_width, features), bf16),
            pltpu.VMEM((chunk_width, features), bf16),
            pltpu.VMEM((query_heads, rows, HEAD_SIZE), bf16),
            pltpu.VMEM((back + 1, rows, rows), f32),
            pltpu.VMEM((back + 1, kv_heads, 2, rows, HEAD_SIZE), bf16),
            pltpu.VMEM((n, chunks, rows, chunk_width), bf16),
            pltpu.VMEM((n, rows, quarter), f32),
            pltpu.VMEM((n, rows, quarter), f32),
            pltpu.VMEM((2 * n - 1, n, rows, quarter), bf16),
            pltpu.VMEM((2 * n - 1, 2, rows, quarter), bf16),
            pltpu.VMEM((2 * n - 1, rows, quarter), bf16),
            pltpu.VMEM((2 * n - 1, rows, quarter), bf16),
            pltpu.VMEM((2 * n - 1, rows, quarter), bf16),
            pltpu.VMEM((n, rows, quarter), bf16),
            pltpu.VMEM((n, rows, quarter), bf16),
            dma((4 + kv_heads,)),
            dma((chunks,)),
            dma((back + 1, kv_heads)),
            dma((back + 1, kv_heads)),
            dma((n, chunks)),
            dma((n, chunks)),
            dma((n, chunks)),
            dma((chunks,)),
            dma((chunks,)),
            dma((chunks,)),
            dma((chunks,)),
            dma((2 * n - 1, 2)),
            dma((2 * n - 1, 2)),
            dma((2 * n - 1,)),
            dma((2 * n - 1,)),
            dma((2 * n - 1,)),
            dma((n,)),
            dma((n,)),
            dma((n,)),
        ],
        compiler_params=pltpu.CompilerParams(collective_id=0, has_side_effects=True),
    )(query_matrix, key_matrix, value_matrix, doc_ids.reshape(tokens // rows, rows), jnp.asarray(table), out_weight)


def solution(mesh):
    in_specs = (
        P(("groups", "ctx"), "tp"),
        P(("groups", "ctx"), "tp"),
        P(("groups", "ctx"), "tp"),
        P("groups"),
        P("tp", "ctx"),
    )
    out_specs = P(("groups", "ctx"), "tp")
    n, groups = mesh.shape["ctx"], mesh.shape["groups"]

    def body(*arrays):
        query_matrix, doc_ids = arrays[0], arrays[3]
        back = key_blocks_back(doc_ids.shape[0], query_matrix.shape[0])
        if n == mesh.shape["tp"] and n == 4 and groups == 2 and back == 2:
            return fused(n, groups, *arrays)
        return on_device(*arrays)

    return jax.shard_map(
        body, mesh=mesh, in_specs=in_specs, out_specs=out_specs, check_vma=False
    )
```

```python
import functools
import math

import jax
import jax.numpy as jnp
import numpy as np
from jax import lax
from jax.experimental import pallas as pl
from jax.experimental.pallas import tpu as pltpu
from jax.sharding import PartitionSpec as P

MESH = pl.DeviceIdType.MESH

HEAD_SIZE = 128


rope_base = 1000000.0

LENT_SHARE = 3 / 16


def rotary_tables(rows, token_positions, heads):
    half_dim = HEAD_SIZE // 2
    frequency = jnp.power(
        jnp.float32(rope_base), -jnp.arange(half_dim, dtype=jnp.float32) * (2.0 / HEAD_SIZE)
    )
    angles = token_positions.astype(jnp.float32)[:, None] * frequency[None, :]
    cosine = jnp.cos(angles)[:, None, :]
    sine = jnp.sin(angles)[:, None, :]
    values = rows.astype(jnp.float32).reshape(rows.shape[0], heads, HEAD_SIZE)
    first = values[..., :half_dim]
    second = values[..., half_dim:]
    turned = jnp.concatenate([first * cosine - second * sine, second * cosine + first * sine], -1)
    return turned.reshape(rows.shape[0], heads * HEAD_SIZE).astype(jnp.bfloat16)


def on_device(query_matrix, key_matrix, value_matrix, doc_ids, out_weight):
    ctx_index = lax.axis_index("ctx")
    tok_rows = query_matrix.shape[0]
    query_heads = query_matrix.shape[1] // HEAD_SIZE
    key_heads = key_matrix.shape[1] // HEAD_SIZE
    group_width = query_heads // key_heads
    inverse_root = HEAD_SIZE ** (-0.5)
    local_rows = jnp.arange(tok_rows, dtype=jnp.int32)
    given_pos = ctx_index * tok_rows + local_rows
    query_matrix_rot = rotary_tables(query_matrix, given_pos, query_heads)
    keys_here = rotary_tables(key_matrix, given_pos, key_heads)
    query_doc = jnp.take(doc_ids, given_pos, axis=0)
    query_four = query_matrix_rot.reshape(tok_rows, key_heads, group_width, HEAD_SIZE)

    def attend(state, block):
        key_block, value_block, doc_block, pos_block = block
        row_max, totals, accum = state
        scores = (
            jnp.einsum("qkgd,skd->kgqs", query_four, key_block, preferred_element_type=jnp.float32)
            * inverse_root
        )
        allowed = (
            (query_doc[:, None] == doc_block[None, :]) & (pos_block[None, :] <= given_pos[:, None])
        )[None, None]
        new_max = jnp.maximum(row_max, jnp.max(jnp.where(allowed, scores, -1e30), -1))
        weights = jnp.where(allowed, jnp.exp(scores - new_max[..., None]), 0.0)
        factor = jnp.exp(row_max - new_max)
        totals = totals * factor + jnp.sum(weights, -1)
        accum = accum * jnp.transpose(factor, (2, 0, 1))[..., None] + jnp.einsum(
            "kgqs,skd->qkgd",
            weights.astype(jnp.bfloat16),
            value_block,
            preferred_element_type=jnp.float32,
        )
        return (new_max, totals, accum)

    start_state = (
        jnp.full((key_heads, group_width, tok_rows), -1e30, jnp.float32),
        jnp.zeros((key_heads, group_width, tok_rows), jnp.float32),
        jnp.zeros((tok_rows, key_heads, group_width, HEAD_SIZE), jnp.float32),
    )
    key_piece = lax.all_gather(keys_here, "ctx", axis=0, tiled=True)
    value_piece = lax.all_gather(value_matrix, "ctx", axis=0, tiled=True)
    count = key_piece.shape[0]
    block_rows = math.gcd(count, 512)
    block_count = count // block_rows
    positions = jnp.arange(count, dtype=jnp.int32)
    blocks = (
        key_piece.reshape(block_count, block_rows, key_heads, HEAD_SIZE),
        value_piece.reshape(block_count, block_rows, key_heads, HEAD_SIZE),
        jnp.take(doc_ids, positions, axis=0).reshape(block_count, block_rows),
        positions.reshape(block_count, block_rows),
    )

    def step_block(inner_state, block):
        return (attend(inner_state, block), None)

    final_state, unused_out = lax.scan(step_block, start_state, blocks)
    row_max, totals, accum = final_state
    attention = (
        (accum / jnp.transpose(totals, (2, 0, 1))[..., None])
        .reshape(tok_rows, query_heads * HEAD_SIZE)
        .astype(jnp.bfloat16)
    )
    terms = jnp.dot(
        attention,
        lax.all_gather(out_weight, "ctx", axis=1, tiled=True),
        preferred_element_type=jnp.float32,
    )
    return lax.psum_scatter(terms.astype(jnp.bfloat16), "tp", scatter_dimension=1, tiled=True)


def fused_kernel(
    n, groups, back, query_ref, key_ref, value_ref, doc_ref, table_ref, weight_ref, out_ref,
    query_in, key_in, table, docs, weight, lent, rotated, bias, kv, gathered, sums,
    partial, pair_in, crossing, cross_in, summed, landed, halves, landed_far, landed_aid,
    load_sem, weight_sem, kv_send, kv_recv, away_send, edge_send, chunk_recv, lend_send, lend_recv,
    share_send, share_recv, pair_send, pair_recv, cross_send, cross_recv, result_send, result_recv,
    half_send, far_recv, aid_recv, store_sem,
):
    group = lax.axis_index("groups")
    ctx = lax.axis_index("ctx")
    tp = lax.axis_index("tp")
    rows = query_ref.shape[0]
    kv_heads = key_ref.shape[1] // HEAD_SIZE
    query_heads = query_ref.shape[1] // HEAD_SIZE
    group_width = query_heads // kv_heads
    ends = chunk_ends(query_heads, groups)
    starts = [0] + ends[:-1]
    chunks = len(ends)
    quarter = partial.shape[3]
    last = n - 1
    lent_chunk = chunks - 1
    pieces = lend_send.shape[0]
    half_rows = lent.shape[0] // groups
    piece_rows = half_rows // pieces

    def columns_of(chunk):
        return pl.ds(starts[chunk] * HEAD_SIZE, (ends[chunk] - starts[chunk]) * HEAD_SIZE)

    is_edge = (ctx == 0) | (ctx == last)
    is_helper = (ctx == 1) | (ctx == last - 1)
    helped = jnp.where(ctx == 1, 0, last)
    other_group = lax.rem(group + 1, groups)
    pair = tp + 1 - 2 * lax.rem(tp, 2)
    across = lax.rem(tp + 2, n)
    pair_across = lax.rem(pair + 2, n)

    def remote(src, dst, send, recv, to_ctx, to_tp):
        return pltpu.make_async_remote_copy(
            src_ref=src, dst_ref=dst, send_sem=send, recv_sem=recv,
            device_id={"ctx": to_ctx, "tp": to_tp}, device_id_type=MESH,
        )

    barrier = pltpu.get_barrier_semaphore()

    def greet(**device):
        pl.semaphore_signal(barrier, inc=1, device_id=device, device_id_type=MESH)

    @pl.when(ctx > 0)
    def _():
        greet(ctx=ctx - 1)

    @pl.when(ctx < last)
    def _():
        greet(ctx=ctx + 1)

    @pl.when(ctx == back)
    def _():
        greet(ctx=ctx - back)

    for step in range(1, n):
        greet(tp=lax.rem(tp + step, n))

    @pl.when(is_helper)
    def _():
        greet(groups=other_group)

    greetings = n - 1 + sum(
        flag.astype(jnp.int32) for flag in (ctx > 0, ctx < last, ctx == 0, is_helper)
    )

    first_row = pl.multiple_of(ctx * rows, rows)
    loads = [
        pltpu.make_async_copy(key_ref, key_in, load_sem.at[0]),
        pltpu.make_async_copy(table_ref.at[:, pl.ds(first_row, rows)], table, load_sem.at[1]),
        pltpu.make_async_copy(doc_ref, docs, load_sem.at[2]),
        pltpu.make_async_copy(query_ref, query_in, load_sem.at[3]),
    ]
    value_loads = [
        pltpu.make_async_copy(
            value_ref.at[:, pl.ds(head * HEAD_SIZE, HEAD_SIZE)], kv.at[back, head, 1], load_sem.at[4 + head]
        )
        for head in range(kv_heads)
    ]
    weight_loads = [
        pltpu.make_async_copy(
            weight_ref.at[columns_of(chunk)], weight.at[columns_of(chunk)], weight_sem.at[chunk]
        )
        for chunk in [lent_chunk] + list(range(lent_chunk))
    ]
    for load in loads + value_loads + weight_loads:
        load.start()

    def turn(values):
        values = values.astype(jnp.float32)
        return (values * table[0] + pltpu.roll(values, HEAD_SIZE // 2, 1) * table[1]).astype(jnp.bfloat16)

    loads[0].wait()
    loads[1].wait()
    for head in range(kv_heads):
        kv[back, head, 0] = turn(key_in[:, head * HEAD_SIZE : (head + 1) * HEAD_SIZE])
    for load in value_loads:
        load.wait()

    for slot in range(back):
        @pl.when(ctx < back - slot)
        def _():
            kv[slot] = jnp.zeros(kv.shape[1:], kv.dtype)

    pl.semaphore_wait(barrier, greetings)

    def kv_copy(slot, head):
        return remote(
            kv.at[slot, head], kv.at[slot - 1, head], kv_send.at[slot, head], kv_recv.at[slot - 1, head],
            lax.rem(ctx + 1, n), tp,
        )

    def kv_direct(head):
        return remote(
            kv.at[back, head], kv.at[0, head], kv_send.at[0, head], kv_recv.at[0, head], lax.rem(ctx + back, n), tp
        )

    for head in range(kv_heads):
        @pl.when(ctx < last)
        def _():
            kv_copy(back, head).start()

        @pl.when(ctx == 0)
        def _():
            kv_direct(head).start()

    def lend_copy(piece):
        start = pl.multiple_of(group * half_rows + piece * piece_rows, piece_rows)
        return remote(
            weight.at[pl.ds(starts[lent_chunk] * HEAD_SIZE + start, piece_rows)], lent.at[pl.ds(start, piece_rows)],
            lend_send.at[piece], lend_recv.at[piece], jnp.where(ctx == 0, 1, last - 1), tp,
        )

    def share_copy(piece, owner):
        start = pl.multiple_of(owner * half_rows + piece * piece_rows, piece_rows)
        here = lent.at[pl.ds(start, piece_rows)]
        return pltpu.make_async_remote_copy(
            src_ref=here, dst_ref=here, send_sem=share_send.at[piece], recv_sem=share_recv.at[piece],
            device_id={"groups": other_group}, device_id_type=MESH,
        )

    weight_loads[0].wait()

    @pl.when(is_edge)
    def _():
        for piece in range(pieces):
            lend_copy(piece).start()

    loads[2].wait()
    own_docs = jnp.broadcast_to(docs[pl.ds(ctx, 1), :], (rows, rows)).astype(jnp.float32).T
    row_index = lax.broadcasted_iota(jnp.int32, (rows, rows), 0)
    column_index = lax.broadcasted_iota(jnp.int32, (rows, rows), 1)
    for slot in range(back + 1):
        block = ctx - back + slot
        their_docs = docs[pl.ds(lax.max(block, 0), 1), :].astype(jnp.float32)
        allowed = (own_docs == their_docs) & (block * rows + column_index <= ctx * rows + row_index) & (block >= 0)
        bias[slot] = jnp.where(allowed, 0.0, -1e30)

    loads[3].wait()
    for head in range(query_heads):
        rotated[head] = turn(query_in[:, head * HEAD_SIZE : (head + 1) * HEAD_SIZE])


    forwards = (ctx >= back) & (ctx < last)

    def take_kv(head):
        kv_copy(back, head).wait_recv()

        @pl.when(forwards)
        def _():
            kv_copy(back - 1, head).start()

    for head in range(kv_heads):
        @pl.when(ctx >= (1 if head == 0 else back))
        def _():
            take_kv(head)

    away = jnp.where(ctx < n // 2, 1, -1)

    def block_at(distance):
        return ctx + distance * away

    def chunk_copy(block, chunk, send, to_ctx):
        here = gathered.at[block, :, columns_of(chunk)]
        return remote(here, here, send.at[block, chunk], chunk_recv.at[block, chunk], to_ctx, tp)

    def away_copy(block, chunk):
        return chunk_copy(block, chunk, away_send, ctx + away)

    def edge_copy(block, chunk):
        return chunk_copy(block, chunk, edge_send, helped)

    scale = HEAD_SIZE ** (-0.5) * math.log2(math.e)
    contract = (((1,), (1,)), ((), ()))
    for head in range(query_heads):
        kv_head = head // group_width
        if head == ends[0]:
            @pl.when((ctx >= 1) & (ctx < back))
            def _():
                for other in range(1, kv_heads):
                    take_kv(other)

        if head % group_width == 0:
            @pl.when(ctx >= back)
            def _():
                kv_copy(1, kv_head).wait_recv()

        scores = [
            lax.dot_general(rotated[head], kv[slot, kv_head, 0], contract, preferred_element_type=jnp.float32) * scale
            + bias[slot]
            for slot in range(back + 1)
        ]
        row_max = functools.reduce(jnp.maximum, scores).max(-1, keepdims=True)
        weights = [jnp.exp2(score - row_max) for score in scores]
        totals = sum(weights).sum(-1, keepdims=True)
        mixed = sum(
            jnp.dot(weights[slot].astype(jnp.bfloat16), kv[slot, kv_head, 1], preferred_element_type=jnp.float32)
            for slot in range(back + 1)
        )
        gathered[ctx, :, head * HEAD_SIZE : (head + 1) * HEAD_SIZE] = (mixed / totals).astype(jnp.bfloat16)
        if head + 1 in ends:
            chunk = ends.index(head + 1)
            away_copy(ctx, chunk).start()
            if chunk != lent_chunk:
                @pl.when(is_helper)
                def _():
                    edge_copy(ctx, chunk).start()

    def pass_on(piece):
        lend_copy(piece).wait_recv()
        share_copy(piece, group).start()

    @pl.when(is_helper)
    def _():
        pass_on(0)
        pass_on(1)

    def pair_copy(place, index):
        return remote(
            partial.at[place, pair_across if index else pair], pair_in.at[place, index],
            pair_send.at[place, index], pair_recv.at[place, index], ctx, pair,
        )

    def cross_copy(place):
        return remote(
            crossing.at[place], cross_in.at[place], cross_send.at[place], cross_recv.at[place], ctx, across
        )

    parts = (pair_across, pair, across, tp)

    def part_columns(part):
        return pl.ds(pl.multiple_of(part * quarter, quarter), quarter)

    def emit(place, index, product):
        partial[place, parts[index]] = product.astype(jnp.bfloat16)
        if index < 2:
            pair_copy(place, 1 - index).start()

    def project(block, chunk, keep, own):
        for index, part in enumerate(parts):
            product = jnp.dot(
                gathered[block, :, columns_of(chunk)], weight[columns_of(chunk), part_columns(part)],
                preferred_element_type=jnp.float32,
            )
            if chunk > 0:
                product = product + sums[keep, index]
            if chunk == lent_chunk:
                emit(block, index, product)
            elif chunk == lent_chunk - 1 and not own:
                @pl.when(is_edge)
                def _():
                    emit(block, index, product)

                @pl.when(jnp.logical_not(is_edge))
                def _():
                    sums[keep, index] = product
            else:
                sums[keep, index] = product

    def cross(place):
        pair_copy(place, 1).wait_recv()
        value = partial[place, across].astype(jnp.float32) + pair_in[place, 1].astype(jnp.float32)
        crossing[place] = value.astype(jnp.bfloat16)
        cross_copy(place).start()

    def collect(place):
        pair_copy(place, 0).wait_recv()
        value = partial[place, tp].astype(jnp.float32) + pair_in[place, 0].astype(jnp.float32)
        cross_copy(place).wait_recv()
        return (value + cross_in[place].astype(jnp.float32)).astype(jnp.bfloat16)

    def result_copy(block):
        return remote(
            summed.at[block], landed.at[tp], result_send.at[block], result_recv.at[tp], block, ctx
        )

    def finish(block):
        value = collect(block)
        mine = (block == ctx) & (tp == ctx)

        @pl.when(mine)
        def _():
            landed[tp] = value

        @pl.when(jnp.logical_not(mine))
        def _():
            summed[block] = value
            result_copy(block).start()

    for load in weight_loads[1:]:
        load.wait()
    for chunk in range(chunks):
        project(ctx, chunk, 0, True)

    def aid_copy(index):
        return remote(
            summed.at[n + index], landed_aid.at[tp], result_send.at[n + index], aid_recv.at[tp],
            block_at(index), helped,
        )

    def far_copy():
        return remote(
            halves, landed_far.at[tp], half_send, far_recv.at[tp], last - ctx, ctx
        )

    def pair_sum(place, index):
        pair_copy(place, index).wait_recv()
        part = across if index else tp
        value = partial[place, part].astype(jnp.float32) + pair_in[place, index].astype(jnp.float32)
        return value.astype(jnp.bfloat16)

    def finish_far(place):
        for index in (1, 0):
            halves[index] = pair_sum(place, index)
        far_copy().start()

    def aid(index):
        for position, part in enumerate(parts):
            product = jnp.dot(
                gathered[block_at(index), :, columns_of(lent_chunk)], lent[:, part_columns(part)],
                preferred_element_type=jnp.float32,
            )
            emit(n + index, position, product)

    def finish_aid(index):
        value = collect(n + index)
        if index == 0:
            @pl.when(tp == helped)
            def _():
                landed_aid[tp] = value

            @pl.when(tp != helped)
            def _():
                summed[n] = value
                aid_copy(0).start()
        else:
            summed[n + index] = value
            aid_copy(index).start()

    def take(block, chunk, forward):
        away_copy(block, chunk).wait_recv()
        if forward is not None:
            forward(block, chunk).start()

    @pl.when(is_edge)
    def _():
        def gather_step(distance, carry):
            block = block_at(distance)
            for chunk in range(lent_chunk):
                take(block, chunk, None)
                project(block, chunk, 1, False)
                if chunk == 0:
                    cross(block_at(distance - 1))
                if chunk == 1:
                    finish(block_at(distance - 1))
            return carry

        lax.fori_loop(1, n, gather_step, 0)
        finish_far(last - ctx)

    @pl.when(is_helper)
    def _():
        def near(chunk):
            take(helped, chunk, away_copy)
            project(helped, chunk, 0, False)

        def far(distance, chunk):
            take(block_at(distance), chunk, edge_copy if chunk < lent_chunk else None)
            project(block_at(distance), chunk, distance, False)

        pass_on(2)
        far(1, 0)
        pass_on(3)
        far(1, 1)
        cross(ctx)
        near(0)
        far(1, 2)
        far(1, lent_chunk)
        near(1)
        finish(ctx)
        near(2)
        cross(block_at(1))
        far(2, 0)
        for piece in range(pieces):
            share_copy(piece, other_group).wait_recv()
        aid(1)
        aid(0)
        far(2, 1)
        cross(n + 1)
        cross(n)
        finish(block_at(1))
        near(lent_chunk)
        far(2, 2)
        cross(helped)
        far(2, lent_chunk)
        aid(2)
        cross(block_at(2))
        cross(n + 2)
        finish_aid(1)
        finish_aid(0)
        finish(helped)
        finish(block_at(2))
        finish_aid(2)

    is_far = is_edge & (tp == last - ctx)
    gets_aid = ((tp == 0) | (tp == last)) & (ctx != tp)
    aid_here = is_helper & (tp == helped)

    @pl.when(is_far)
    def _():
        for part in range(n):
            far = far_recv.at[part]
            remote(halves, landed_far.at[part], half_send, far, ctx, part).wait_recv()

    @pl.when(gets_aid)
    def _():
        for part in range(n):
            @pl.when(jnp.logical_not(aid_here & (tp == part)))
            def _():
                here = aid_recv.at[part]
                remote(summed.at[n], landed_aid.at[part], result_send.at[n], here, ctx, part).wait_recv()

    def both_halves(landing, part):
        return landing[part, 0].astype(jnp.float32) + landing[(part + 2) % n, 1].astype(jnp.float32)

    for part in range(n):
        @pl.when(jnp.logical_not(is_far | ((tp == ctx) & (tp == part))))
        def _():
            remote(
                summed.at[0], landed.at[part], result_send.at[0], result_recv.at[part], ctx, part
            ).wait_recv()

        @pl.when(is_far)
        def _():
            whole = both_halves(landed_far, part) + landed_aid[part].astype(jnp.float32)
            landed[part] = whole.astype(jnp.bfloat16)

        @pl.when(gets_aid & jnp.logical_not(is_far))
        def _():
            whole = landed[part].astype(jnp.float32) + landed_aid[part].astype(jnp.float32)
            landed[part] = whole.astype(jnp.bfloat16)

        pltpu.make_async_copy(
            landed.at[part], out_ref.at[:, pl.ds(part * quarter, quarter)], store_sem.at[part]
        ).start()

    for head in range(kv_heads):
        @pl.when(ctx < last)
        def _():
            kv_copy(back, head).wait_send()

        @pl.when(ctx == 0)
        def _():
            kv_direct(head).wait_send()

        @pl.when(forwards)
        def _():
            kv_copy(back - 1, head).wait_send()

    for piece in range(pieces):
        @pl.when(is_edge)
        def _():
            lend_copy(piece).wait_send()

        @pl.when(is_helper)
        def _():
            share_copy(piece, group).wait_send()

    def drain(block, carry):
        for chunk in range(chunks):
            @pl.when((block == ctx) | (is_helper & (block == helped)))
            def _():
                away_copy(block, chunk).wait_send()

            if chunk < lent_chunk:
                @pl.when(is_helper & (block != helped))
                def _():
                    edge_copy(block, chunk).wait_send()

        for index in range(2):
            pair_copy(block, index).wait_send()

        far_block = is_edge & (block == last - ctx)

        @pl.when(jnp.logical_not(far_block))
        def _():
            cross_copy(block).wait_send()

        @pl.when(jnp.logical_not(far_block | ((block == ctx) & (tp == ctx))))
        def _():
            result_copy(block).wait_send()

        return carry

    lax.fori_loop(0, n, drain, 0)

    @pl.when(is_edge)
    def _():
        far_copy().wait_send()

    @pl.when(is_helper)
    def _():
        for index in range(n - 1):
            for side in range(2):
                pair_copy(n + index, side).wait_send()
            cross_copy(n + index).wait_send()
            if index == 0:
                @pl.when(tp != helped)
                def _():
                    aid_copy(0).wait_send()
            else:
                aid_copy(index).wait_send()

    for part in range(n):
        pltpu.make_async_copy(
            landed.at[part], out_ref.at[:, pl.ds(part * quarter, quarter)], store_sem.at[part]
        ).wait()


def chunk_ends(heads, groups):
    lent = max(1, round(heads * LENT_SHARE))
    kept = heads - lent
    return [heads // 4, heads // 2, kept, heads]


def key_blocks_back(tokens, rows):
    return -(-(tokens // 2 - 1) // rows)


def fused(n, groups, query_matrix, key_matrix, value_matrix, doc_ids, out_weight):
    rows, query_width = query_matrix.shape
    query_heads, kv_heads = query_width // HEAD_SIZE, key_matrix.shape[1] // HEAD_SIZE
    features = out_weight.shape[1]
    tokens = doc_ids.shape[0]
    back = key_blocks_back(tokens, rows)
    chunks = len(chunk_ends(query_heads, groups))
    lent_rows = query_width - chunk_ends(query_heads, groups)[-2] * HEAD_SIZE
    pieces = 4
    quarter = features // n
    half = HEAD_SIZE // 2
    frequency = np.power(np.float32(rope_base), -np.arange(half, dtype=np.float32) * np.float32(2.0 / HEAD_SIZE))
    angles = np.arange(tokens, dtype=np.float32)[:, None] * frequency[None, :]
    cosine, sine = np.cos(angles), np.sin(angles)
    table = np.stack([np.concatenate([cosine, cosine], 1), np.concatenate([-sine, sine], 1)]).astype(np.float32)
    any_space = pl.BlockSpec(memory_space=pl.ANY)
    bf16, f32, dma = jnp.bfloat16, jnp.float32, pltpu.SemaphoreType.DMA
    return pl.pallas_call(
        functools.partial(fused_kernel, n, groups, back),
        out_shape=jax.ShapeDtypeStruct((rows, features), bf16),
        in_specs=[any_space] * 6,
        out_specs=any_space,
        scratch_shapes=[
            pltpu.VMEM((rows, query_width), bf16),
            pltpu.VMEM((rows, kv_heads * HEAD_SIZE), bf16),
            pltpu.VMEM((2, rows, HEAD_SIZE), f32),
            pltpu.VMEM((tokens // rows, rows), jnp.int32),
            pltpu.VMEM((query_width, features), bf16),
            pltpu.VMEM((lent_rows, features), bf16),
            pltpu.VMEM((query_heads, rows, HEAD_SIZE), bf16),
            pltpu.VMEM((back + 1, rows, rows), f32),
            pltpu.VMEM((back + 1, kv_heads, 2, rows, HEAD_SIZE), bf16),
            pltpu.VMEM((n, rows, query_width), bf16),
            pltpu.VMEM((3, n, rows, quarter), f32),
            pltpu.VMEM((2 * n - 1, n, rows, quarter), bf16),
            pltpu.VMEM((2 * n - 1, 2, rows, quarter), bf16),
            pltpu.VMEM((2 * n - 1, rows, quarter), bf16),
            pltpu.VMEM((2 * n - 1, rows, quarter), bf16),
            pltpu.VMEM((2 * n - 1, rows, quarter), bf16),
            pltpu.VMEM((n, rows, quarter), bf16),
            pltpu.VMEM((2, rows, quarter), bf16),
            pltpu.VMEM((n, 2, rows, quarter), bf16),
            pltpu.VMEM((n, rows, quarter), bf16),
            dma((4 + kv_heads,)),
            dma((chunks,)),
            dma((back + 1, kv_heads)),
            dma((back + 1, kv_heads)),
            dma((n, chunks)),
            dma((n, chunks)),
            dma((n, chunks)),
            dma((pieces,)),
            dma((pieces,)),
            dma((pieces,)),
            dma((pieces,)),
            dma((2 * n - 1, 2)),
            dma((2 * n - 1, 2)),
            dma((2 * n - 1,)),
            dma((2 * n - 1,)),
            dma((2 * n - 1,)),
            dma((n,)),
            dma,
            dma((n,)),
            dma((n,)),
            dma((n,)),
        ],
        compiler_params=pltpu.CompilerParams(collective_id=0, has_side_effects=True),
    )(query_matrix, key_matrix, value_matrix, doc_ids.reshape(tokens // rows, rows), jnp.asarray(table), out_weight)


def solution(mesh):
    in_specs = (
        P(("groups", "ctx"), "tp"),
        P(("groups", "ctx"), "tp"),
        P(("groups", "ctx"), "tp"),
        P("groups"),
        P("tp", "ctx"),
    )
    out_specs = P(("groups", "ctx"), "tp")
    n, groups = mesh.shape["ctx"], mesh.shape["groups"]

    def body(*arrays):
        query_matrix, doc_ids = arrays[0], arrays[3]
        back = key_blocks_back(doc_ids.shape[0], query_matrix.shape[0])
        if n == mesh.shape["tp"] and n == 4 and groups == 2 and back == 2:
            return fused(n, groups, *arrays)
        return on_device(*arrays)

    return jax.shard_map(
        body, mesh=mesh, in_specs=in_specs, out_specs=out_specs, check_vma=False
    )
```

```python
import functools
import math

import jax
import jax.numpy as jnp
import numpy as np
from jax import lax
from jax.experimental import pallas as pl
from jax.experimental.pallas import tpu as pltpu
from jax.sharding import PartitionSpec as P

MESH = pl.DeviceIdType.MESH

HEAD_SIZE = 128


rope_base = 1000000.0

LENT_SHARE = 3 / 16


def rotary_tables(rows, token_positions, heads):
    half_dim = HEAD_SIZE // 2
    frequency = jnp.power(
        jnp.float32(rope_base), -jnp.arange(half_dim, dtype=jnp.float32) * (2.0 / HEAD_SIZE)
    )
    angles = token_positions.astype(jnp.float32)[:, None] * frequency[None, :]
    cosine = jnp.cos(angles)[:, None, :]
    sine = jnp.sin(angles)[:, None, :]
    values = rows.astype(jnp.float32).reshape(rows.shape[0], heads, HEAD_SIZE)
    first = values[..., :half_dim]
    second = values[..., half_dim:]
    turned = jnp.concatenate([first * cosine - second * sine, second * cosine + first * sine], -1)
    return turned.reshape(rows.shape[0], heads * HEAD_SIZE).astype(jnp.bfloat16)


def on_device(query_matrix, key_matrix, value_matrix, doc_ids, out_weight):
    ctx_index = lax.axis_index("ctx")
    tok_rows = query_matrix.shape[0]
    query_heads = query_matrix.shape[1] // HEAD_SIZE
    key_heads = key_matrix.shape[1] // HEAD_SIZE
    group_width = query_heads // key_heads
    inverse_root = HEAD_SIZE ** (-0.5)
    local_rows = jnp.arange(tok_rows, dtype=jnp.int32)
    given_pos = ctx_index * tok_rows + local_rows
    query_matrix_rot = rotary_tables(query_matrix, given_pos, query_heads)
    keys_here = rotary_tables(key_matrix, given_pos, key_heads)
    query_doc = jnp.take(doc_ids, given_pos, axis=0)
    query_four = query_matrix_rot.reshape(tok_rows, key_heads, group_width, HEAD_SIZE)

    def attend(state, block):
        key_block, value_block, doc_block, pos_block = block
        row_max, totals, accum = state
        scores = (
            jnp.einsum("qkgd,skd->kgqs", query_four, key_block, preferred_element_type=jnp.float32)
            * inverse_root
        )
        allowed = (
            (query_doc[:, None] == doc_block[None, :]) & (pos_block[None, :] <= given_pos[:, None])
        )[None, None]
        new_max = jnp.maximum(row_max, jnp.max(jnp.where(allowed, scores, -1e30), -1))
        weights = jnp.where(allowed, jnp.exp(scores - new_max[..., None]), 0.0)
        factor = jnp.exp(row_max - new_max)
        totals = totals * factor + jnp.sum(weights, -1)
        accum = accum * jnp.transpose(factor, (2, 0, 1))[..., None] + jnp.einsum(
            "kgqs,skd->qkgd",
            weights.astype(jnp.bfloat16),
            value_block,
            preferred_element_type=jnp.float32,
        )
        return (new_max, totals, accum)

    start_state = (
        jnp.full((key_heads, group_width, tok_rows), -1e30, jnp.float32),
        jnp.zeros((key_heads, group_width, tok_rows), jnp.float32),
        jnp.zeros((tok_rows, key_heads, group_width, HEAD_SIZE), jnp.float32),
    )
    key_piece = lax.all_gather(keys_here, "ctx", axis=0, tiled=True)
    value_piece = lax.all_gather(value_matrix, "ctx", axis=0, tiled=True)
    count = key_piece.shape[0]
    block_rows = math.gcd(count, 512)
    block_count = count // block_rows
    positions = jnp.arange(count, dtype=jnp.int32)
    blocks = (
        key_piece.reshape(block_count, block_rows, key_heads, HEAD_SIZE),
        value_piece.reshape(block_count, block_rows, key_heads, HEAD_SIZE),
        jnp.take(doc_ids, positions, axis=0).reshape(block_count, block_rows),
        positions.reshape(block_count, block_rows),
    )

    def step_block(inner_state, block):
        return (attend(inner_state, block), None)

    final_state, unused_out = lax.scan(step_block, start_state, blocks)
    row_max, totals, accum = final_state
    attention = (
        (accum / jnp.transpose(totals, (2, 0, 1))[..., None])
        .reshape(tok_rows, query_heads * HEAD_SIZE)
        .astype(jnp.bfloat16)
    )
    terms = jnp.dot(
        attention,
        lax.all_gather(out_weight, "ctx", axis=1, tiled=True),
        preferred_element_type=jnp.float32,
    )
    return lax.psum_scatter(terms.astype(jnp.bfloat16), "tp", scatter_dimension=1, tiled=True)


def fused_kernel(
    n, groups, back, query_ref, key_ref, value_ref, doc_ref, table_ref, weight_ref, out_ref,
    query_in, key_in, table, docs, weight, lent, rotated, bias, kv, gathered, sums,
    partial, pair_in, crossing, cross_in, summed, landed, halves, landed_far, landed_aid,
    load_sem, weight_sem, kv_send, kv_recv, away_send, edge_send, chunk_recv, lend_send, lend_recv,
    share_send, share_recv, pair_send, pair_recv, cross_send, cross_recv, result_send, result_recv,
    half_send, far_recv, aid_recv,
):
    group = lax.axis_index("groups")
    ctx = lax.axis_index("ctx")
    tp = lax.axis_index("tp")
    rows = query_ref.shape[0]
    kv_heads = key_ref.shape[1] // HEAD_SIZE
    query_heads = query_ref.shape[1] // HEAD_SIZE
    group_width = query_heads // kv_heads
    ends = chunk_ends(query_heads, groups)
    starts = [0] + ends[:-1]
    chunks = len(ends)
    quarter = partial.shape[3]
    last = n - 1
    lent_chunk = chunks - 1
    pieces = lend_send.shape[0]
    half_rows = lent.shape[0] // groups
    piece_rows = half_rows // pieces

    def columns_of(chunk):
        return pl.ds(starts[chunk] * HEAD_SIZE, (ends[chunk] - starts[chunk]) * HEAD_SIZE)

    is_edge = (ctx == 0) | (ctx == last)
    is_helper = (ctx == 1) | (ctx == last - 1)
    helped = jnp.where(ctx == 1, 0, last)
    other_group = lax.rem(group + 1, groups)
    pair = tp + 1 - 2 * lax.rem(tp, 2)
    across = lax.rem(tp + 2, n)
    pair_across = lax.rem(pair + 2, n)

    def remote(src, dst, send, recv, to_ctx, to_tp):
        return pltpu.make_async_remote_copy(
            src_ref=src, dst_ref=dst, send_sem=send, recv_sem=recv,
            device_id={"ctx": to_ctx, "tp": to_tp}, device_id_type=MESH,
        )

    barrier = pltpu.get_barrier_semaphore()

    def greet(**device):
        pl.semaphore_signal(barrier, inc=1, device_id=device, device_id_type=MESH)

    @pl.when(ctx > 0)
    def _():
        greet(ctx=ctx - 1)

    @pl.when(ctx < last)
    def _():
        greet(ctx=ctx + 1)

    @pl.when(ctx == back)
    def _():
        greet(ctx=ctx - back)

    for step in range(1, n):
        greet(tp=lax.rem(tp + step, n))

    @pl.when(is_helper)
    def _():
        greet(groups=other_group)

    greetings = n - 1 + sum(
        flag.astype(jnp.int32) for flag in (ctx > 0, ctx < last, ctx == 0, is_helper)
    )

    first_row = pl.multiple_of(ctx * rows, rows)
    loads = [
        pltpu.make_async_copy(key_ref, key_in, load_sem.at[0]),
        pltpu.make_async_copy(table_ref.at[:, pl.ds(first_row, rows)], table, load_sem.at[1]),
        pltpu.make_async_copy(doc_ref, docs, load_sem.at[2]),
        pltpu.make_async_copy(query_ref, query_in, load_sem.at[3]),
    ]
    value_loads = [
        pltpu.make_async_copy(
            value_ref.at[:, pl.ds(head * HEAD_SIZE, HEAD_SIZE)], kv.at[back, head, 1], load_sem.at[4 + head]
        )
        for head in range(kv_heads)
    ]
    weight_loads = [
        pltpu.make_async_copy(
            weight_ref.at[columns_of(chunk)], weight.at[columns_of(chunk)], weight_sem.at[chunk]
        )
        for chunk in [lent_chunk] + list(range(lent_chunk))
    ]
    for load in loads + value_loads + weight_loads:
        load.start()

    def turn(values):
        values = values.astype(jnp.float32)
        return (values * table[0] + pltpu.roll(values, HEAD_SIZE // 2, 1) * table[1]).astype(jnp.bfloat16)

    loads[0].wait()
    loads[1].wait()
    for head in range(kv_heads):
        kv[back, head, 0] = turn(key_in[:, head * HEAD_SIZE : (head + 1) * HEAD_SIZE])
    for load in value_loads:
        load.wait()

    for slot in range(back):
        @pl.when(ctx < back - slot)
        def _():
            kv[slot] = jnp.zeros(kv.shape[1:], kv.dtype)

    pl.semaphore_wait(barrier, greetings)

    def kv_copy(slot, head):
        return remote(
            kv.at[slot, head], kv.at[slot - 1, head], kv_send.at[slot, head], kv_recv.at[slot - 1, head],
            lax.rem(ctx + 1, n), tp,
        )

    def kv_direct(head):
        return remote(
            kv.at[back, head], kv.at[0, head], kv_send.at[0, head], kv_recv.at[0, head], lax.rem(ctx + back, n), tp
        )

    for head in range(kv_heads):
        @pl.when(ctx < last)
        def _():
            kv_copy(back, head).start()

        if head == 0:
            @pl.when(ctx == 0)
            def _():
                kv_direct(head).start()

    def lend_copy(piece):
        start = pl.multiple_of(group * half_rows + piece * piece_rows, piece_rows)
        return remote(
            weight.at[pl.ds(starts[lent_chunk] * HEAD_SIZE + start, piece_rows)], lent.at[pl.ds(start, piece_rows)],
            lend_send.at[piece], lend_recv.at[piece], jnp.where(ctx == 0, 1, last - 1), tp,
        )

    def share_copy(piece, owner):
        start = pl.multiple_of(owner * half_rows + piece * piece_rows, piece_rows)
        here = lent.at[pl.ds(start, piece_rows)]
        return pltpu.make_async_remote_copy(
            src_ref=here, dst_ref=here, send_sem=share_send.at[piece], recv_sem=share_recv.at[piece],
            device_id={"groups": other_group}, device_id_type=MESH,
        )

    weight_loads[0].wait()

    @pl.when(is_edge)
    def _():
        for piece in range(pieces):
            lend_copy(piece).start()

    loads[2].wait()
    own_docs = jnp.broadcast_to(docs[pl.ds(ctx, 1), :], (rows, rows)).astype(jnp.float32).T
    row_index = lax.broadcasted_iota(jnp.int32, (rows, rows), 0)
    column_index = lax.broadcasted_iota(jnp.int32, (rows, rows), 1)
    for slot in range(back + 1):
        block = ctx - back + slot
        their_docs = docs[pl.ds(lax.max(block, 0), 1), :].astype(jnp.float32)
        allowed = (own_docs == their_docs) & (block * rows + column_index <= ctx * rows + row_index) & (block >= 0)
        bias[slot] = jnp.where(allowed, 0.0, -1e30)

    loads[3].wait()
    for head in range(query_heads):
        rotated[head] = turn(query_in[:, head * HEAD_SIZE : (head + 1) * HEAD_SIZE])


    def forwards(head):
        return (ctx >= (back if head == 0 else back - 1)) & (ctx < last)

    def take_kv(head):
        kv_copy(back, head).wait_recv()

        @pl.when(forwards(head))
        def _():
            kv_copy(back - 1, head).start()

    for head in range(kv_heads):
        @pl.when(ctx >= (1 if head == 0 else back))
        def _():
            take_kv(head)

    away = jnp.where(ctx < n // 2, 1, -1)

    def block_at(distance):
        return ctx + distance * away

    def chunk_copy(block, chunk, send, to_ctx):
        here = gathered.at[block, :, columns_of(chunk)]
        return remote(here, here, send.at[block, chunk], chunk_recv.at[block, chunk], to_ctx, tp)

    def away_copy(block, chunk):
        return chunk_copy(block, chunk, away_send, ctx + away)

    def edge_copy(block, chunk):
        return chunk_copy(block, chunk, edge_send, helped)

    scale = HEAD_SIZE ** (-0.5) * math.log2(math.e)
    contract = (((1,), (1,)), ((), ()))
    for head in range(query_heads):
        kv_head = head // group_width
        if head == ends[1] - 1:
            @pl.when((ctx >= 1) & (ctx < back))
            def _():
                for other in range(1, kv_heads):
                    take_kv(other)

        if head % group_width == 0:
            @pl.when(ctx >= back)
            def _():
                kv_copy(1, kv_head).wait_recv()

        scores = [
            lax.dot_general(rotated[head], kv[slot, kv_head, 0], contract, preferred_element_type=jnp.float32) * scale
            + bias[slot]
            for slot in range(back + 1)
        ]
        row_max = functools.reduce(jnp.maximum, scores).max(-1, keepdims=True)
        weights = [jnp.exp2(score - row_max) for score in scores]
        totals = sum(weights).sum(-1, keepdims=True)
        mixed = sum(
            jnp.dot(weights[slot].astype(jnp.bfloat16), kv[slot, kv_head, 1], preferred_element_type=jnp.float32)
            for slot in range(back + 1)
        )
        gathered[ctx, :, head * HEAD_SIZE : (head + 1) * HEAD_SIZE] = (mixed / totals).astype(jnp.bfloat16)
        if head + 1 in ends:
            chunk = ends.index(head + 1)
            away_copy(ctx, chunk).start()
            if chunk != lent_chunk:
                @pl.when(is_helper)
                def _():
                    edge_copy(ctx, chunk).start()

    def pass_on(piece):
        lend_copy(piece).wait_recv()
        share_copy(piece, group).start()

    @pl.when(is_helper)
    def _():
        pass_on(0)
        pass_on(1)

    def pair_copy(place, index):
        return remote(
            partial.at[place, pair_across if index else pair], pair_in.at[place, index],
            pair_send.at[place, index], pair_recv.at[place, index], ctx, pair,
        )

    def cross_copy(place):
        return remote(
            crossing.at[place], cross_in.at[place], cross_send.at[place], cross_recv.at[place], ctx, across
        )

    parts = (pair_across, pair, across, tp)

    def part_columns(part):
        return pl.ds(pl.multiple_of(part * quarter, quarter), quarter)

    def emit(place, index, product):
        partial[place, parts[index]] = product.astype(jnp.bfloat16)
        if index < 2:
            pair_copy(place, 1 - index).start()

    def project(block, chunk, keep, own):
        for index, part in enumerate(parts):
            product = jnp.dot(
                gathered[block, :, columns_of(chunk)], weight[columns_of(chunk), part_columns(part)],
                preferred_element_type=jnp.float32,
            )
            if chunk > 0:
                product = product + sums[keep, index]
            if chunk == lent_chunk:
                emit(block, index, product)
            elif chunk == lent_chunk - 1 and not own:
                @pl.when(is_edge)
                def _():
                    emit(block, index, product)

                @pl.when(jnp.logical_not(is_edge))
                def _():
                    sums[keep, index] = product
            else:
                sums[keep, index] = product

    def cross(place):
        pair_copy(place, 1).wait_recv()
        value = partial[place, across].astype(jnp.float32) + pair_in[place, 1].astype(jnp.float32)
        crossing[place] = value.astype(jnp.bfloat16)
        cross_copy(place).start()

    def collect(place):
        pair_copy(place, 0).wait_recv()
        value = partial[place, tp].astype(jnp.float32) + pair_in[place, 0].astype(jnp.float32)
        cross_copy(place).wait_recv()
        return (value + cross_in[place].astype(jnp.float32)).astype(jnp.bfloat16)

    def result_copy(block):
        return remote(
            summed.at[block], landed.at[tp], result_send.at[block], result_recv.at[tp], block, ctx
        )

    def finish(block):
        value = collect(block)
        mine = (block == ctx) & (tp == ctx)

        @pl.when(mine)
        def _():
            landed[tp] = value

        @pl.when(jnp.logical_not(mine))
        def _():
            summed[block] = value
            result_copy(block).start()

    for load in weight_loads[1:]:
        load.wait()
    for chunk in range(chunks):
        project(ctx, chunk, 0, True)

    def aid_copy(index):
        return remote(
            summed.at[n + index], landed_aid.at[tp], result_send.at[n + index], aid_recv.at[tp],
            block_at(index), helped,
        )

    far_block = jnp.where(ctx < n // 2, last, 0)
    sends_far = ctx != 1

    def far_copy():
        return remote(
            halves, landed_far.at[tp], half_send, far_recv.at[tp], far_block, ctx
        )

    def pair_sum(place, index):
        pair_copy(place, index).wait_recv()
        part = across if index else tp
        value = partial[place, part].astype(jnp.float32) + pair_in[place, index].astype(jnp.float32)
        return value.astype(jnp.bfloat16)

    def finish_far():
        for index in (1, 0):
            halves[index] = pair_sum(far_block, index)
        far_copy().start()

    def aid(index):
        for position, part in enumerate(parts):
            product = jnp.dot(
                gathered[block_at(index), :, columns_of(lent_chunk)], lent[:, part_columns(part)],
                preferred_element_type=jnp.float32,
            )
            emit(n + index, position, product)

    def finish_aid(index):
        value = collect(n + index)
        if index == 0:
            @pl.when(tp == helped)
            def _():
                landed_aid[tp] = value

            @pl.when(tp != helped)
            def _():
                summed[n] = value
                aid_copy(0).start()
        else:
            summed[n + index] = value
            aid_copy(index).start()

    def take(block, chunk, forward):
        away_copy(block, chunk).wait_recv()
        if forward is not None:
            forward(block, chunk).start()

    @pl.when(is_edge)
    def _():
        def gather_step(distance, carry):
            block = block_at(distance)
            for chunk in range(lent_chunk):
                if chunk == lent_chunk - 1:
                    finish(block_at(distance - 1))
                take(block, chunk, None)
                project(block, chunk, 1, False)
                if chunk == 0:
                    cross(block_at(distance - 1))
            return carry

        lax.fori_loop(1, n, gather_step, 0)
        finish_far()

    def near(chunk):
        take(helped, chunk, away_copy)
        project(helped, chunk, 0, False)

    def far(distance, chunk):
        take(block_at(distance), chunk, edge_copy if chunk < lent_chunk else None)
        project(block_at(distance), chunk, distance, False)

    def aid_both():
        for piece in range(pieces):
            share_copy(piece, other_group).wait_recv()
        aid(1)
        aid(0)

    def last_chunks():
        far(2, lent_chunk)
        aid(2)
        cross(n + 2)

    @pl.when(ctx == 1)
    def _():
        far(1, 0)
        pass_on(2)
        far(1, 1)
        pass_on(3)
        cross(ctx)
        near(0)
        far(1, 2)
        far(1, 3)
        near(1)
        finish(ctx)
        far(1, lent_chunk)
        near(2)
        cross(block_at(1))
        far(2, 0)
        aid_both()
        near(3)
        far(2, 1)
        cross(n + 1)
        cross(n)
        near(lent_chunk)
        far(2, 2)
        finish(block_at(1))
        cross(helped)
        far(2, 3)
        finish_aid(1)
        last_chunks()
        cross(far_block)
        finish_aid(0)
        finish(helped)
        finish_aid(2)
        finish(far_block)

    @pl.when(ctx == last - 1)
    def _():
        pass_on(2)
        far(1, 0)
        pass_on(3)
        near(0)
        far(1, 1)
        cross(ctx)
        near(1)
        far(1, 2)
        far(1, 3)
        near(2)
        far(1, lent_chunk)
        finish(ctx)
        near(3)
        cross(block_at(1))
        near(lent_chunk)
        aid_both()
        far(2, 0)
        cross(helped)
        cross(n + 1)
        cross(n)
        far(2, 1)
        far(2, 2)
        finish(block_at(1))
        finish(helped)
        far(2, 3)
        finish_aid(1)
        last_chunks()
        finish_far()
        finish_aid(0)
        finish_aid(2)

    is_far = ((ctx == 0) & (tp >= n // 2)) | ((ctx == last) & (tp == 0))
    gets_aid = ((tp == 0) | (tp == last)) & (ctx != tp)
    aid_here = is_helper & (tp == helped)

    @pl.when(is_far)
    def _():
        for part in range(n):
            far = far_recv.at[part]
            remote(halves, landed_far.at[part], half_send, far, ctx, part).wait_recv()

    @pl.when(gets_aid)
    def _():
        for part in range(n):
            @pl.when(jnp.logical_not(aid_here & (tp == part)))
            def _():
                here = aid_recv.at[part]
                remote(summed.at[n], landed_aid.at[part], result_send.at[n], here, ctx, part).wait_recv()

    def both_halves(landing, part):
        return landing[part, 0].astype(jnp.float32) + landing[(part + 2) % n, 1].astype(jnp.float32)

    for part in range(n):
        @pl.when(jnp.logical_not(is_far | ((tp == ctx) & (tp == part))))
        def _():
            remote(
                summed.at[0], landed.at[part], result_send.at[0], result_recv.at[part], ctx, part
            ).wait_recv()

        columns = pl.ds(part * quarter, quarter)

        @pl.when(is_far & jnp.logical_not(gets_aid))
        def _():
            out_ref[:, columns] = both_halves(landed_far, part).astype(jnp.bfloat16)

        @pl.when(is_far & gets_aid)
        def _():
            whole = both_halves(landed_far, part) + landed_aid[part].astype(jnp.float32)
            out_ref[:, columns] = whole.astype(jnp.bfloat16)

        @pl.when(gets_aid & jnp.logical_not(is_far))
        def _():
            whole = landed[part].astype(jnp.float32) + landed_aid[part].astype(jnp.float32)
            out_ref[:, columns] = whole.astype(jnp.bfloat16)

        @pl.when(jnp.logical_not(gets_aid | is_far))
        def _():
            out_ref[:, columns] = landed[part]

    for head in range(kv_heads):
        @pl.when(ctx < last)
        def _():
            kv_copy(back, head).wait_send()

        if head == 0:
            @pl.when(ctx == 0)
            def _():
                kv_direct(head).wait_send()

        @pl.when(forwards(head))
        def _():
            kv_copy(back - 1, head).wait_send()

    for piece in range(pieces):
        @pl.when(is_edge)
        def _():
            lend_copy(piece).wait_send()

        @pl.when(is_helper)
        def _():
            share_copy(piece, group).wait_send()

    def drain(block, carry):
        for chunk in range(chunks):
            @pl.when((block == ctx) | (is_helper & (block == helped)))
            def _():
                away_copy(block, chunk).wait_send()

            if chunk < lent_chunk:
                @pl.when(is_helper & (block != helped))
                def _():
                    edge_copy(block, chunk).wait_send()

        for index in range(2):
            pair_copy(block, index).wait_send()

        @pl.when((block != far_block) | jnp.logical_not(sends_far))
        def _():
            cross_copy(block).wait_send()

        own_part = (block == ctx) & (tp == ctx)

        @pl.when(((block != far_block) | jnp.logical_not(sends_far)) & jnp.logical_not(own_part))
        def _():
            result_copy(block).wait_send()

        return carry

    lax.fori_loop(0, n, drain, 0)

    @pl.when(sends_far)
    def _():
        far_copy().wait_send()

    @pl.when(is_helper)
    def _():
        for index in range(n - 1):
            for side in range(2):
                pair_copy(n + index, side).wait_send()
            cross_copy(n + index).wait_send()
            if index == 0:
                @pl.when(tp != helped)
                def _():
                    aid_copy(0).wait_send()
            else:
                aid_copy(index).wait_send()


def chunk_ends(heads, groups):
    lent = max(1, round(heads * LENT_SHARE))
    kept = heads - lent
    return [heads // 8, heads * 3 // 8, heads * 5 // 8, kept, heads]


def key_blocks_back(tokens, rows):
    return -(-(tokens // 2 - 1) // rows)


def fused(n, groups, query_matrix, key_matrix, value_matrix, doc_ids, out_weight):
    rows, query_width = query_matrix.shape
    query_heads, kv_heads = query_width // HEAD_SIZE, key_matrix.shape[1] // HEAD_SIZE
    features = out_weight.shape[1]
    tokens = doc_ids.shape[0]
    back = key_blocks_back(tokens, rows)
    chunks = len(chunk_ends(query_heads, groups))
    lent_rows = query_width - chunk_ends(query_heads, groups)[-2] * HEAD_SIZE
    pieces = 4
    quarter = features // n
    half = HEAD_SIZE // 2
    frequency = np.power(np.float32(rope_base), -np.arange(half, dtype=np.float32) * np.float32(2.0 / HEAD_SIZE))
    angles = np.arange(tokens, dtype=np.float32)[:, None] * frequency[None, :]
    cosine, sine = np.cos(angles), np.sin(angles)
    table = np.stack([np.concatenate([cosine, cosine], 1), np.concatenate([-sine, sine], 1)]).astype(np.float32)
    any_space = pl.BlockSpec(memory_space=pl.ANY)
    bf16, f32, dma = jnp.bfloat16, jnp.float32, pltpu.SemaphoreType.DMA
    return pl.pallas_call(
        functools.partial(fused_kernel, n, groups, back),
        out_shape=pltpu.VMEM((rows, features), bf16),
        in_specs=[any_space] * 6,
        out_specs=pl.BlockSpec(memory_space=pltpu.VMEM),
        scratch_shapes=[
            pltpu.VMEM((rows, query_width), bf16),
            pltpu.VMEM((rows, kv_heads * HEAD_SIZE), bf16),
            pltpu.VMEM((2, rows, HEAD_SIZE), f32),
            pltpu.VMEM((tokens // rows, rows), jnp.int32),
            pltpu.VMEM((query_width, features), bf16),
            pltpu.VMEM((lent_rows, features), bf16),
            pltpu.VMEM((query_heads, rows, HEAD_SIZE), bf16),
            pltpu.VMEM((back + 1, rows, rows), f32),
            pltpu.VMEM((back + 1, kv_heads, 2, rows, HEAD_SIZE), bf16),
            pltpu.VMEM((n, rows, query_width), bf16),
            pltpu.VMEM((3, n, rows, quarter), f32),
            pltpu.VMEM((2 * n - 1, n, rows, quarter), bf16),
            pltpu.VMEM((2 * n - 1, 2, rows, quarter), bf16),
            pltpu.VMEM((2 * n - 1, rows, quarter), bf16),
            pltpu.VMEM((2 * n - 1, rows, quarter), bf16),
            pltpu.VMEM((2 * n - 1, rows, quarter), bf16),
            pltpu.VMEM((n, rows, quarter), bf16),
            pltpu.VMEM((2, rows, quarter), bf16),
            pltpu.VMEM((n, 2, rows, quarter), bf16),
            pltpu.VMEM((n, rows, quarter), bf16),
            dma((4 + kv_heads,)),
            dma((chunks,)),
            dma((back + 1, kv_heads)),
            dma((back + 1, kv_heads)),
            dma((n, chunks)),
            dma((n, chunks)),
            dma((n, chunks)),
            dma((pieces,)),
            dma((pieces,)),
            dma((pieces,)),
            dma((pieces,)),
            dma((2 * n - 1, 2)),
            dma((2 * n - 1, 2)),
            dma((2 * n - 1,)),
            dma((2 * n - 1,)),
            dma((2 * n - 1,)),
            dma((n,)),
            dma,
            dma((n,)),
            dma((n,)),
        ],
        compiler_params=pltpu.CompilerParams(collective_id=0, has_side_effects=True),
    )(query_matrix, key_matrix, value_matrix, doc_ids.reshape(tokens // rows, rows), jnp.asarray(table), out_weight)


def solution(mesh):
    in_specs = (
        P(("groups", "ctx"), "tp"),
        P(("groups", "ctx"), "tp"),
        P(("groups", "ctx"), "tp"),
        P("groups"),
        P("tp", "ctx"),
    )
    out_specs = P(("groups", "ctx"), "tp")
    n, groups = mesh.shape["ctx"], mesh.shape["groups"]

    def body(*arrays):
        query_matrix, doc_ids = arrays[0], arrays[3]
        back = key_blocks_back(doc_ids.shape[0], query_matrix.shape[0])
        if n == mesh.shape["tp"] and n == 4 and groups == 2 and back == 2:
            return fused(n, groups, *arrays)
        return on_device(*arrays)

    return jax.shard_map(
        body, mesh=mesh, in_specs=in_specs, out_specs=out_specs, check_vma=False
    )
```

```python
import functools
import math

import jax
import jax.numpy as jnp
import numpy as np
from jax import lax
from jax.experimental import pallas as pl
from jax.experimental.pallas import tpu as pltpu
from jax.sharding import PartitionSpec as P

MESH = pl.DeviceIdType.MESH

HEAD_SIZE = 128


rope_base = 1000000.0

LENT_SHARE = 3 / 16


def rotary_tables(rows, token_positions, heads):
    half_dim = HEAD_SIZE // 2
    frequency = jnp.power(
        jnp.float32(rope_base), -jnp.arange(half_dim, dtype=jnp.float32) * (2.0 / HEAD_SIZE)
    )
    angles = token_positions.astype(jnp.float32)[:, None] * frequency[None, :]
    cosine = jnp.cos(angles)[:, None, :]
    sine = jnp.sin(angles)[:, None, :]
    values = rows.astype(jnp.float32).reshape(rows.shape[0], heads, HEAD_SIZE)
    first = values[..., :half_dim]
    second = values[..., half_dim:]
    turned = jnp.concatenate([first * cosine - second * sine, second * cosine + first * sine], -1)
    return turned.reshape(rows.shape[0], heads * HEAD_SIZE).astype(jnp.bfloat16)


def on_device(query_matrix, key_matrix, value_matrix, doc_ids, out_weight):
    ctx_index = lax.axis_index("ctx")
    tok_rows = query_matrix.shape[0]
    query_heads = query_matrix.shape[1] // HEAD_SIZE
    key_heads = key_matrix.shape[1] // HEAD_SIZE
    group_width = query_heads // key_heads
    inverse_root = HEAD_SIZE ** (-0.5)
    local_rows = jnp.arange(tok_rows, dtype=jnp.int32)
    given_pos = ctx_index * tok_rows + local_rows
    query_matrix_rot = rotary_tables(query_matrix, given_pos, query_heads)
    keys_here = rotary_tables(key_matrix, given_pos, key_heads)
    query_doc = jnp.take(doc_ids, given_pos, axis=0)
    query_four = query_matrix_rot.reshape(tok_rows, key_heads, group_width, HEAD_SIZE)

    def attend(state, block):
        key_block, value_block, doc_block, pos_block = block
        row_max, totals, accum = state
        scores = (
            jnp.einsum("qkgd,skd->kgqs", query_four, key_block, preferred_element_type=jnp.float32)
            * inverse_root
        )
        allowed = (
            (query_doc[:, None] == doc_block[None, :]) & (pos_block[None, :] <= given_pos[:, None])
        )[None, None]
        new_max = jnp.maximum(row_max, jnp.max(jnp.where(allowed, scores, -1e30), -1))
        weights = jnp.where(allowed, jnp.exp(scores - new_max[..., None]), 0.0)
        factor = jnp.exp(row_max - new_max)
        totals = totals * factor + jnp.sum(weights, -1)
        accum = accum * jnp.transpose(factor, (2, 0, 1))[..., None] + jnp.einsum(
            "kgqs,skd->qkgd",
            weights.astype(jnp.bfloat16),
            value_block,
            preferred_element_type=jnp.float32,
        )
        return (new_max, totals, accum)

    start_state = (
        jnp.full((key_heads, group_width, tok_rows), -1e30, jnp.float32),
        jnp.zeros((key_heads, group_width, tok_rows), jnp.float32),
        jnp.zeros((tok_rows, key_heads, group_width, HEAD_SIZE), jnp.float32),
    )
    key_piece = lax.all_gather(keys_here, "ctx", axis=0, tiled=True)
    value_piece = lax.all_gather(value_matrix, "ctx", axis=0, tiled=True)
    count = key_piece.shape[0]
    block_rows = math.gcd(count, 512)
    block_count = count // block_rows
    positions = jnp.arange(count, dtype=jnp.int32)
    blocks = (
        key_piece.reshape(block_count, block_rows, key_heads, HEAD_SIZE),
        value_piece.reshape(block_count, block_rows, key_heads, HEAD_SIZE),
        jnp.take(doc_ids, positions, axis=0).reshape(block_count, block_rows),
        positions.reshape(block_count, block_rows),
    )

    def step_block(inner_state, block):
        return (attend(inner_state, block), None)

    final_state, unused_out = lax.scan(step_block, start_state, blocks)
    row_max, totals, accum = final_state
    attention = (
        (accum / jnp.transpose(totals, (2, 0, 1))[..., None])
        .reshape(tok_rows, query_heads * HEAD_SIZE)
        .astype(jnp.bfloat16)
    )
    terms = jnp.dot(
        attention,
        lax.all_gather(out_weight, "ctx", axis=1, tiled=True),
        preferred_element_type=jnp.float32,
    )
    return lax.psum_scatter(terms.astype(jnp.bfloat16), "tp", scatter_dimension=1, tiled=True)


def fused_kernel(
    n, groups, back, query_ref, key_ref, value_ref, doc_ref, table_ref, weight_ref, out_ref,
    query_in, key_in, table, docs, weight, lent, rotated, bias, kv, gathered, sums,
    partial, pair_in, crossing, cross_in, summed, landed, halves, landed_far, landed_aid,
    load_sem, weight_sem, kv_send, kv_recv, away_send, edge_send, chunk_recv, lend_send, lend_recv,
    share_send, share_recv, pair_send, pair_recv, cross_send, cross_recv, result_send, result_recv,
    half_send, far_recv, aid_recv,
):
    group = lax.axis_index("groups")
    ctx = lax.axis_index("ctx")
    tp = lax.axis_index("tp")
    rows = query_ref.shape[0]
    kv_heads = key_ref.shape[1] // HEAD_SIZE
    query_heads = query_ref.shape[1] // HEAD_SIZE
    group_width = query_heads // kv_heads
    ends = chunk_ends(query_heads, groups)
    starts = [0] + ends[:-1]
    chunks = len(ends)
    quarter = partial.shape[3]
    last = n - 1
    lent_chunk = chunks - 1
    pieces = lend_recv.shape[0]
    half_rows = lent.shape[0] // groups
    piece_rows = half_rows // pieces

    def columns_of(chunk):
        return pl.ds(starts[chunk] * HEAD_SIZE, (ends[chunk] - starts[chunk]) * HEAD_SIZE)

    is_edge = (ctx == 0) | (ctx == last)
    is_helper = (ctx == 1) | (ctx == last - 1)
    helped = jnp.where(ctx == 1, 0, last)
    other_group = lax.rem(group + 1, groups)
    pair = tp + 1 - 2 * lax.rem(tp, 2)
    across = lax.rem(tp + 2, n)
    pair_across = lax.rem(pair + 2, n)

    def remote(src, dst, send, recv, to_ctx, to_tp):
        return pltpu.make_async_remote_copy(
            src_ref=src, dst_ref=dst, send_sem=send, recv_sem=recv,
            device_id={"ctx": to_ctx, "tp": to_tp}, device_id_type=MESH,
        )

    barrier = pltpu.get_barrier_semaphore()

    def greet(**device):
        pl.semaphore_signal(barrier, inc=1, device_id=device, device_id_type=MESH)

    @pl.when(ctx > 0)
    def _():
        greet(ctx=ctx - 1)

    @pl.when(ctx < last)
    def _():
        greet(ctx=ctx + 1)

    @pl.when(ctx == back)
    def _():
        greet(ctx=ctx - back)

    for step in range(1, n):
        greet(tp=lax.rem(tp + step, n))

    @pl.when(is_helper)
    def _():
        greet(groups=other_group)

    greetings = n - 1 + sum(
        flag.astype(jnp.int32) for flag in (ctx > 0, ctx < last, ctx == 0, is_helper)
    )

    first_row = pl.multiple_of(ctx * rows, rows)
    loads = [
        pltpu.make_async_copy(key_ref, key_in, load_sem.at[0]),
        pltpu.make_async_copy(table_ref.at[:, pl.ds(first_row, rows)], table, load_sem.at[1]),
        pltpu.make_async_copy(doc_ref, docs, load_sem.at[2]),
        pltpu.make_async_copy(query_ref, query_in, load_sem.at[3]),
    ]
    value_loads = [
        pltpu.make_async_copy(
            value_ref.at[:, pl.ds(head * HEAD_SIZE, HEAD_SIZE)], kv.at[back, head, 1], load_sem.at[4 + head]
        )
        for head in range(kv_heads)
    ]
    lent_start = starts[lent_chunk] * HEAD_SIZE
    weight_rows = [pl.ds(lent_start, lent.shape[0]), pl.ds(0, lent_start)]
    weight_loads = [
        pltpu.make_async_copy(weight_ref.at[part], weight.at[part], weight_sem.at[index])
        for index, part in enumerate(weight_rows)
    ]
    for load in loads + value_loads + weight_loads:
        load.start()

    def turn(values):
        values = values.astype(jnp.float32)
        return (values * table[0] + pltpu.roll(values, HEAD_SIZE // 2, 1) * table[1]).astype(jnp.bfloat16)

    loads[0].wait()
    loads[1].wait()
    for head in range(kv_heads):
        kv[back, head, 0] = turn(key_in[:, head * HEAD_SIZE : (head + 1) * HEAD_SIZE])
    for load in value_loads:
        load.wait()

    for slot in range(back):
        @pl.when(ctx < back - slot)
        def _():
            kv[slot] = jnp.zeros(kv.shape[1:], kv.dtype)

    pl.semaphore_wait(barrier, greetings)

    def kv_copy(slot, head):
        return remote(
            kv.at[slot, head], kv.at[slot - 1, head], kv_send.at[slot, head], kv_recv.at[slot - 1, head],
            lax.rem(ctx + 1, n), tp,
        )

    def kv_direct(head):
        return remote(
            kv.at[back, head], kv.at[0, head], kv_send.at[0, head], kv_recv.at[0, head], lax.rem(ctx + back, n), tp
        )

    for head in range(kv_heads):
        @pl.when(ctx < last)
        def _():
            kv_copy(back, head).start()

        if head == 0:
            @pl.when(ctx == 0)
            def _():
                kv_direct(head).start()

    def lend_copy(piece):
        start = pl.multiple_of(group * half_rows + piece * piece_rows, piece_rows)
        return remote(
            weight.at[pl.ds(starts[lent_chunk] * HEAD_SIZE + start, piece_rows)], lent.at[pl.ds(start, piece_rows)],
            lend_send, lend_recv.at[piece], jnp.where(ctx == 0, 1, last - 1), tp,
        )

    def share_copy(piece, owner):
        start = pl.multiple_of(owner * half_rows + piece * piece_rows, piece_rows)
        here = lent.at[pl.ds(start, piece_rows)]
        return pltpu.make_async_remote_copy(
            src_ref=here, dst_ref=here, send_sem=share_send, recv_sem=share_recv,
            device_id={"groups": other_group}, device_id_type=MESH,
        )

    weight_loads[0].wait()

    @pl.when(is_edge)
    def _():
        for piece in range(pieces):
            lend_copy(piece).start()

    loads[2].wait()
    own_docs = jnp.broadcast_to(docs[pl.ds(ctx, 1), :], (rows, rows)).astype(jnp.float32).T
    row_index = lax.broadcasted_iota(jnp.int32, (rows, rows), 0)
    column_index = lax.broadcasted_iota(jnp.int32, (rows, rows), 1)
    for slot in range(back + 1):
        block = ctx - back + slot
        their_docs = docs[pl.ds(lax.max(block, 0), 1), :].astype(jnp.float32)
        allowed = (own_docs == their_docs) & (block * rows + column_index <= ctx * rows + row_index) & (block >= 0)
        bias[slot] = jnp.where(allowed, 0.0, -1e30)

    loads[3].wait()
    for head in range(query_heads):
        rotated[head] = turn(query_in[:, head * HEAD_SIZE : (head + 1) * HEAD_SIZE])


    def forwards(head):
        return (ctx >= (back if head == 0 else back - 1)) & (ctx < last)

    def take_kv(head):
        kv_copy(back, head).wait_recv()

        @pl.when(forwards(head))
        def _():
            kv_copy(back - 1, head).start()

    for head in range(kv_heads):
        @pl.when(ctx >= (1 if head == 0 else back))
        def _():
            take_kv(head)

    away = jnp.where(ctx < n // 2, 1, -1)

    def block_at(distance):
        return ctx + distance * away

    def chunk_copy(block, chunk, send, to_ctx):
        here = gathered.at[block, :, columns_of(chunk)]
        return remote(here, here, send, chunk_recv.at[block, chunk], to_ctx, tp)

    def away_copy(block, chunk):
        return chunk_copy(block, chunk, away_send.at[jnp.where(block == ctx, 0, 1)], ctx + away)

    def edge_copy(block, chunk):
        return chunk_copy(block, chunk, edge_send.at[(block - ctx) * away], helped)

    scale = HEAD_SIZE ** (-0.5) * math.log2(math.e)
    contract = (((1,), (1,)), ((), ()))
    for head in range(query_heads):
        kv_head = head // group_width
        if head == ends[1] - 1:
            @pl.when((ctx >= 1) & (ctx < back))
            def _():
                for other in range(1, kv_heads):
                    take_kv(other)

        if head % group_width == 0:
            @pl.when(ctx >= back)
            def _():
                kv_copy(1, kv_head).wait_recv()

        scores = [
            lax.dot_general(rotated[head], kv[slot, kv_head, 0], contract, preferred_element_type=jnp.float32) * scale
            + bias[slot]
            for slot in range(back + 1)
        ]
        row_max = functools.reduce(jnp.maximum, scores).max(-1, keepdims=True)
        weights = [jnp.exp2(score - row_max) for score in scores]
        totals = sum(weights).sum(-1, keepdims=True)
        mixed = sum(
            jnp.dot(weights[slot].astype(jnp.bfloat16), kv[slot, kv_head, 1], preferred_element_type=jnp.float32)
            for slot in range(back + 1)
        )
        gathered[ctx, :, head * HEAD_SIZE : (head + 1) * HEAD_SIZE] = (mixed / totals).astype(jnp.bfloat16)
        if head + 1 in ends:
            chunk = ends.index(head + 1)
            away_copy(ctx, chunk).start()
            if chunk != lent_chunk:
                @pl.when(is_helper)
                def _():
                    edge_copy(ctx, chunk).start()

    def pass_on(piece):
        lend_copy(piece).wait_recv()
        share_copy(piece, group).start()

    @pl.when(is_helper)
    def _():
        pass_on(0)
        pass_on(1)

    def pair_copy(place, index):
        return remote(
            partial.at[place, pair_across if index else pair], pair_in.at[place, index],
            pair_send, pair_recv.at[place, index], ctx, pair,
        )

    def cross_copy(place):
        return remote(
            crossing.at[place], cross_in.at[place], cross_send, cross_recv.at[place], ctx, across
        )

    parts = (pair_across, pair, across, tp)

    def part_columns(part):
        return pl.ds(pl.multiple_of(part * quarter, quarter), quarter)

    def emit(place, index, product):
        partial[place, parts[index]] = product.astype(jnp.bfloat16)
        if index < 2:
            pair_copy(place, 1 - index).start()

    def project(block, chunk, keep, own):
        for index, part in enumerate(parts):
            product = jnp.dot(
                gathered[block, :, columns_of(chunk)], weight[columns_of(chunk), part_columns(part)],
                preferred_element_type=jnp.float32,
            )
            if chunk > 0:
                product = product + sums[keep, index]
            if chunk == lent_chunk:
                emit(block, index, product)
            elif chunk == lent_chunk - 1 and not own:
                @pl.when(is_edge)
                def _():
                    emit(block, index, product)

                @pl.when(jnp.logical_not(is_edge))
                def _():
                    sums[keep, index] = product
            else:
                sums[keep, index] = product

    def cross(place):
        pair_copy(place, 1).wait_recv()
        value = partial[place, across].astype(jnp.float32) + pair_in[place, 1].astype(jnp.float32)
        crossing[place] = value.astype(jnp.bfloat16)
        cross_copy(place).start()

    def collect(place):
        pair_copy(place, 0).wait_recv()
        value = partial[place, tp].astype(jnp.float32) + pair_in[place, 0].astype(jnp.float32)
        cross_copy(place).wait_recv()
        return (value + cross_in[place].astype(jnp.float32)).astype(jnp.bfloat16)

    def result_copy(block):
        return remote(
            summed.at[block], landed.at[tp], result_send.at[block], result_recv, block, ctx
        )

    def finish(block):
        value = collect(block)
        mine = (block == ctx) & (tp == ctx)

        @pl.when(mine)
        def _():
            landed[tp] = value

        @pl.when(jnp.logical_not(mine))
        def _():
            summed[block] = value
            result_copy(block).start()

    for load in weight_loads[1:]:
        load.wait()
    for chunk in range(chunks):
        project(ctx, chunk, 0, True)

    def aid_copy(index):
        return remote(
            summed.at[n + index], landed_aid.at[tp], result_send.at[n + index], aid_recv,
            block_at(index), helped,
        )

    far_block = jnp.where(ctx < n // 2, last, 0)
    sends_far = ctx != 1

    def far_copy():
        return remote(
            halves, landed_far.at[tp], half_send, far_recv, far_block, ctx
        )

    def pair_sum(place, index):
        pair_copy(place, index).wait_recv()
        part = across if index else tp
        value = partial[place, part].astype(jnp.float32) + pair_in[place, index].astype(jnp.float32)
        return value.astype(jnp.bfloat16)

    def finish_far():
        for index in (1, 0):
            halves[index] = pair_sum(far_block, index)
        far_copy().start()

    def aid(index):
        for position, part in enumerate(parts):
            product = jnp.dot(
                gathered[block_at(index), :, columns_of(lent_chunk)], lent[:, part_columns(part)],
                preferred_element_type=jnp.float32,
            )
            emit(n + index, position, product)

    def finish_aid(index):
        value = collect(n + index)
        if index == 0:
            @pl.when(tp == helped)
            def _():
                landed_aid[tp] = value

            @pl.when(tp != helped)
            def _():
                summed[n] = value
                aid_copy(0).start()
        else:
            summed[n + index] = value
            aid_copy(index).start()

    def take(block, chunk, forward):
        away_copy(block, chunk).wait_recv()
        if forward is not None:
            forward(block, chunk).start()

    @pl.when(is_edge)
    def _():
        def gather_step(distance, carry):
            block = block_at(distance)
            for chunk in range(lent_chunk):
                if chunk == lent_chunk - 1:
                    finish(block_at(distance - 1))
                take(block, chunk, None)
                project(block, chunk, 1, False)
                if chunk == 0:
                    cross(block_at(distance - 1))
            return carry

        lax.fori_loop(1, n, gather_step, 0)
        finish_far()

    def near(chunk):
        take(helped, chunk, away_copy)
        project(helped, chunk, 0, False)

    def far(distance, chunk):
        take(block_at(distance), chunk, edge_copy if chunk < lent_chunk else None)
        project(block_at(distance), chunk, distance, False)

    def aid_both():
        arrived = lent.at[pl.ds(pl.multiple_of(other_group * half_rows, half_rows), half_rows)]
        remote(arrived, arrived, share_send, share_recv, ctx, pair).wait_recv()
        aid(1)
        aid(0)

    def last_chunks():
        far(2, lent_chunk)
        aid(2)
        cross(n + 2)

    @pl.when(ctx == 1)
    def _():
        far(1, 0)
        pass_on(2)
        far(1, 1)
        pass_on(3)
        cross(ctx)
        near(0)
        far(1, 2)
        far(1, 3)
        near(1)
        finish(ctx)
        far(1, lent_chunk)
        near(2)
        cross(block_at(1))
        far(2, 0)
        aid_both()
        near(3)
        far(2, 1)
        cross(n + 1)
        cross(n)
        near(lent_chunk)
        far(2, 2)
        finish(block_at(1))
        cross(helped)
        far(2, 3)
        finish_aid(1)
        last_chunks()
        cross(far_block)
        finish_aid(0)
        finish(helped)
        finish_aid(2)
        finish(far_block)

    @pl.when(ctx == last - 1)
    def _():
        pass_on(2)
        far(1, 0)
        pass_on(3)
        near(0)
        far(1, 1)
        cross(ctx)
        near(1)
        far(1, 2)
        far(1, 3)
        near(2)
        far(1, lent_chunk)
        finish(ctx)
        near(3)
        cross(block_at(1))
        near(lent_chunk)
        aid_both()
        far(2, 0)
        cross(helped)
        cross(n + 1)
        cross(n)
        far(2, 1)
        far(2, 2)
        finish(block_at(1))
        finish(helped)
        far(2, 3)
        finish_aid(1)
        last_chunks()
        finish_far()
        finish_aid(0)
        finish_aid(2)

    is_far = ((ctx == 0) & (tp >= n // 2)) | ((ctx == last) & (tp == 0))
    gets_aid = ((tp == 0) | (tp == last)) & (ctx != tp)
    aid_here = is_helper & (tp == helped)

    def landed_all(landing, recv, local):
        if local is None:
            return remote(landing, landing, half_send, recv, ctx, pair).wait_recv()

        @pl.when(local)
        def _():
            some = landing.at[pl.ds(0, n - 1)]
            remote(some, some, half_send, recv, ctx, pair).wait_recv()

        @pl.when(jnp.logical_not(local))
        def _():
            remote(landing, landing, half_send, recv, ctx, pair).wait_recv()

    @pl.when(is_far)
    def _():
        landed_all(landed_far, far_recv, None)

    @pl.when(jnp.logical_not(is_far))
    def _():
        landed_all(landed, result_recv, tp == ctx)

    @pl.when(gets_aid)
    def _():
        landed_all(landed_aid, aid_recv, aid_here)

    def both_halves(landing, part):
        return landing[part, 0].astype(jnp.float32) + landing[(part + 2) % n, 1].astype(jnp.float32)

    for part in range(n):
        columns = pl.ds(part * quarter, quarter)

        @pl.when(is_far & jnp.logical_not(gets_aid))
        def _():
            out_ref[:, columns] = both_halves(landed_far, part).astype(jnp.bfloat16)

        @pl.when(is_far & gets_aid)
        def _():
            whole = both_halves(landed_far, part) + landed_aid[part].astype(jnp.float32)
            out_ref[:, columns] = whole.astype(jnp.bfloat16)

        @pl.when(gets_aid & jnp.logical_not(is_far))
        def _():
            whole = landed[part].astype(jnp.float32) + landed_aid[part].astype(jnp.float32)
            out_ref[:, columns] = whole.astype(jnp.bfloat16)

        @pl.when(jnp.logical_not(gets_aid | is_far))
        def _():
            out_ref[:, columns] = landed[part]

    for head in range(kv_heads):
        @pl.when(ctx < last)
        def _():
            kv_copy(back, head).wait_send()

        if head == 0:
            @pl.when(ctx == 0)
            def _():
                kv_direct(head).wait_send()

        @pl.when(forwards(head))
        def _():
            kv_copy(back - 1, head).wait_send()

    def sent(source, send):
        remote(source, source, send, chunk_recv.at[0, 0], ctx, pair).wait_send()

    half_lent = lent.at[pl.ds(0, half_rows)]
    sent(gathered.at[ctx], away_send.at[0])

    @pl.when(is_edge)
    def _():
        sent(half_lent, lend_send)
        sent(pair_in.at[pl.ds(0, n)], pair_send)
        sent(cross_in.at[pl.ds(0, n - 1)], cross_send)

    @pl.when(is_helper)
    def _():
        sent(half_lent, share_send)
        sent(gathered.at[helped], away_send.at[1])
        sent(pair_in, pair_send)
        for distance in range(n - 1):
            sent(gathered.at[block_at(distance), :, pl.ds(0, starts[lent_chunk] * HEAD_SIZE)], edge_send.at[distance])

    @pl.when(ctx == 1)
    def _():
        sent(cross_in, cross_send)

    @pl.when(ctx == last - 1)
    def _():
        sent(cross_in.at[pl.ds(0, 2 * n - 2)], cross_send)

    def drain(block, carry):
        own_part = (block == ctx) & (tp == ctx)

        @pl.when(((block != far_block) | jnp.logical_not(sends_far)) & jnp.logical_not(own_part))
        def _():
            result_copy(block).wait_send()

        return carry

    lax.fori_loop(0, n, drain, 0)

    @pl.when(sends_far)
    def _():
        far_copy().wait_send()

    @pl.when(is_helper)
    def _():
        for index in range(n - 1):
            if index == 0:
                @pl.when(tp != helped)
                def _():
                    aid_copy(0).wait_send()
            else:
                aid_copy(index).wait_send()


def chunk_ends(heads, groups):
    lent = max(1, round(heads * LENT_SHARE))
    kept = heads - lent
    return [heads // 8, heads * 3 // 8, heads * 5 // 8, kept, heads]


def key_blocks_back(tokens, rows):
    return -(-(tokens // 2 - 1) // rows)


def fused(n, groups, query_matrix, key_matrix, value_matrix, doc_ids, out_weight):
    rows, query_width = query_matrix.shape
    query_heads, kv_heads = query_width // HEAD_SIZE, key_matrix.shape[1] // HEAD_SIZE
    features = out_weight.shape[1]
    tokens = doc_ids.shape[0]
    back = key_blocks_back(tokens, rows)
    chunks = len(chunk_ends(query_heads, groups))
    lent_rows = query_width - chunk_ends(query_heads, groups)[-2] * HEAD_SIZE
    pieces = 4
    quarter = features // n
    half = HEAD_SIZE // 2
    frequency = np.power(np.float32(rope_base), -np.arange(half, dtype=np.float32) * np.float32(2.0 / HEAD_SIZE))
    angles = np.arange(tokens, dtype=np.float32)[:, None] * frequency[None, :]
    cosine, sine = np.cos(angles), np.sin(angles)
    table = np.stack([np.concatenate([cosine, cosine], 1), np.concatenate([-sine, sine], 1)]).astype(np.float32)
    any_space = pl.BlockSpec(memory_space=pl.ANY)
    bf16, f32, dma = jnp.bfloat16, jnp.float32, pltpu.SemaphoreType.DMA
    return pl.pallas_call(
        functools.partial(fused_kernel, n, groups, back),
        out_shape=pltpu.VMEM((rows, features), bf16),
        in_specs=[any_space] * 6,
        out_specs=pl.BlockSpec(memory_space=pltpu.VMEM),
        scratch_shapes=[
            pltpu.VMEM((rows, query_width), bf16),
            pltpu.VMEM((rows, kv_heads * HEAD_SIZE), bf16),
            pltpu.VMEM((2, rows, HEAD_SIZE), f32),
            pltpu.VMEM((tokens // rows, rows), jnp.int32),
            pltpu.VMEM((query_width, features), bf16),
            pltpu.VMEM((lent_rows, features), bf16),
            pltpu.VMEM((query_heads, rows, HEAD_SIZE), bf16),
            pltpu.VMEM((back + 1, rows, rows), f32),
            pltpu.VMEM((back + 1, kv_heads, 2, rows, HEAD_SIZE), bf16),
            pltpu.VMEM((n, rows, query_width), bf16),
            pltpu.VMEM((3, n, rows, quarter), f32),
            pltpu.VMEM((2 * n - 1, n, rows, quarter), bf16),
            pltpu.VMEM((2 * n - 1, 2, rows, quarter), bf16),
            pltpu.VMEM((2 * n - 1, rows, quarter), bf16),
            pltpu.VMEM((2 * n - 1, rows, quarter), bf16),
            pltpu.VMEM((2 * n - 1, rows, quarter), bf16),
            pltpu.VMEM((n, rows, quarter), bf16),
            pltpu.VMEM((2, rows, quarter), bf16),
            pltpu.VMEM((n, 2, rows, quarter), bf16),
            pltpu.VMEM((n, rows, quarter), bf16),
            dma((4 + kv_heads,)),
            dma((2,)),
            dma((back + 1, kv_heads)),
            dma((back, kv_heads)),
            dma((2,)),
            dma((n - 1,)),
            dma((n, chunks)),
            dma,
            dma((pieces,)),
            dma,
            dma,
            dma,
            dma((2 * n - 1, 2)),
            dma,
            dma((2 * n - 1,)),
            dma((2 * n - 1,)),
            dma,
            dma,
            dma,
            dma,
        ],
        compiler_params=pltpu.CompilerParams(collective_id=0, has_side_effects=True),
    )(query_matrix, key_matrix, value_matrix, doc_ids.reshape(tokens // rows, rows), jnp.asarray(table), out_weight)


def solution(mesh):
    in_specs = (
        P(("groups", "ctx"), "tp"),
        P(("groups", "ctx"), "tp"),
        P(("groups", "ctx"), "tp"),
        P("groups"),
        P("tp", "ctx"),
    )
    out_specs = P(("groups", "ctx"), "tp")
    n, groups = mesh.shape["ctx"], mesh.shape["groups"]

    def body(*arrays):
        query_matrix, doc_ids = arrays[0], arrays[3]
        back = key_blocks_back(doc_ids.shape[0], query_matrix.shape[0])
        if n == mesh.shape["tp"] and n == 4 and groups == 2 and back == 2:
            return fused(n, groups, *arrays)
        return on_device(*arrays)

    return jax.shard_map(
        body, mesh=mesh, in_specs=in_specs, out_specs=out_specs, check_vma=False
    )
```

```python
import functools
import math

import jax
import jax.numpy as jnp
import numpy as np
from jax import lax
from jax.experimental import pallas as pl
from jax.experimental.pallas import tpu as pltpu
from jax.sharding import PartitionSpec as P

MESH = pl.DeviceIdType.MESH

HEAD_SIZE = 128


rope_base = 1000000.0

LENT_SHARE = 3 / 16


def rotary_tables(rows, token_positions, heads):
    half_dim = HEAD_SIZE // 2
    frequency = jnp.power(
        jnp.float32(rope_base), -jnp.arange(half_dim, dtype=jnp.float32) * (2.0 / HEAD_SIZE)
    )
    angles = token_positions.astype(jnp.float32)[:, None] * frequency[None, :]
    cosine = jnp.cos(angles)[:, None, :]
    sine = jnp.sin(angles)[:, None, :]
    values = rows.astype(jnp.float32).reshape(rows.shape[0], heads, HEAD_SIZE)
    first = values[..., :half_dim]
    second = values[..., half_dim:]
    turned = jnp.concatenate([first * cosine - second * sine, second * cosine + first * sine], -1)
    return turned.reshape(rows.shape[0], heads * HEAD_SIZE).astype(jnp.bfloat16)


def on_device(query_matrix, key_matrix, value_matrix, doc_ids, out_weight):
    ctx_index = lax.axis_index("ctx")
    tok_rows = query_matrix.shape[0]
    query_heads = query_matrix.shape[1] // HEAD_SIZE
    key_heads = key_matrix.shape[1] // HEAD_SIZE
    group_width = query_heads // key_heads
    inverse_root = HEAD_SIZE ** (-0.5)
    local_rows = jnp.arange(tok_rows, dtype=jnp.int32)
    given_pos = ctx_index * tok_rows + local_rows
    query_matrix_rot = rotary_tables(query_matrix, given_pos, query_heads)
    keys_here = rotary_tables(key_matrix, given_pos, key_heads)
    query_doc = jnp.take(doc_ids, given_pos, axis=0)
    query_four = query_matrix_rot.reshape(tok_rows, key_heads, group_width, HEAD_SIZE)

    def attend(state, block):
        key_block, value_block, doc_block, pos_block = block
        row_max, totals, accum = state
        scores = (
            jnp.einsum("qkgd,skd->kgqs", query_four, key_block, preferred_element_type=jnp.float32)
            * inverse_root
        )
        allowed = (
            (query_doc[:, None] == doc_block[None, :]) & (pos_block[None, :] <= given_pos[:, None])
        )[None, None]
        new_max = jnp.maximum(row_max, jnp.max(jnp.where(allowed, scores, -1e30), -1))
        weights = jnp.where(allowed, jnp.exp(scores - new_max[..., None]), 0.0)
        factor = jnp.exp(row_max - new_max)
        totals = totals * factor + jnp.sum(weights, -1)
        accum = accum * jnp.transpose(factor, (2, 0, 1))[..., None] + jnp.einsum(
            "kgqs,skd->qkgd",
            weights.astype(jnp.bfloat16),
            value_block,
            preferred_element_type=jnp.float32,
        )
        return (new_max, totals, accum)

    start_state = (
        jnp.full((key_heads, group_width, tok_rows), -1e30, jnp.float32),
        jnp.zeros((key_heads, group_width, tok_rows), jnp.float32),
        jnp.zeros((tok_rows, key_heads, group_width, HEAD_SIZE), jnp.float32),
    )
    key_piece = lax.all_gather(keys_here, "ctx", axis=0, tiled=True)
    value_piece = lax.all_gather(value_matrix, "ctx", axis=0, tiled=True)
    count = key_piece.shape[0]
    block_rows = math.gcd(count, 512)
    block_count = count // block_rows
    positions = jnp.arange(count, dtype=jnp.int32)
    blocks = (
        key_piece.reshape(block_count, block_rows, key_heads, HEAD_SIZE),
        value_piece.reshape(block_count, block_rows, key_heads, HEAD_SIZE),
        jnp.take(doc_ids, positions, axis=0).reshape(block_count, block_rows),
        positions.reshape(block_count, block_rows),
    )

    def step_block(inner_state, block):
        return (attend(inner_state, block), None)

    final_state, unused_out = lax.scan(step_block, start_state, blocks)
    row_max, totals, accum = final_state
    attention = (
        (accum / jnp.transpose(totals, (2, 0, 1))[..., None])
        .reshape(tok_rows, query_heads * HEAD_SIZE)
        .astype(jnp.bfloat16)
    )
    terms = jnp.dot(
        attention,
        lax.all_gather(out_weight, "ctx", axis=1, tiled=True),
        preferred_element_type=jnp.float32,
    )
    return lax.psum_scatter(terms.astype(jnp.bfloat16), "tp", scatter_dimension=1, tiled=True)


def fused_kernel(
    n, groups, back, query_ref, key_ref, value_ref, doc_ref, table_ref, weight_ref, out_ref,
    query_in, key_in, table, docs, weight, lent, rotated, bias, kv, gathered, sums,
    partial, pair_in, crossing, cross_in, summed, landed, halves, landed_far, landed_aid,
    load_sem, weight_sem, kv_send, kv_recv, away_send, edge_send, chunk_recv, lend_send, lend_recv,
    share_send, share_recv, pair_send, pair_recv, cross_send, cross_recv, result_send, result_recv,
    half_send, far_recv, aid_recv,
):
    group = lax.axis_index("groups")
    ctx = lax.axis_index("ctx")
    tp = lax.axis_index("tp")
    rows = query_ref.shape[0]
    kv_heads = key_ref.shape[1] // HEAD_SIZE
    query_heads = query_ref.shape[1] // HEAD_SIZE
    group_width = query_heads // kv_heads
    ends = chunk_ends(query_heads, groups)
    starts = [0] + ends[:-1]
    chunks = len(ends)
    quarter = partial.shape[3]
    last = n - 1
    lent_chunk = chunks - 1
    pieces = lend_recv.shape[0]
    half_rows = lent.shape[0] // groups
    piece_rows = half_rows // pieces

    def columns_of(chunk):
        return pl.ds(starts[chunk] * HEAD_SIZE, (ends[chunk] - starts[chunk]) * HEAD_SIZE)

    is_edge = (ctx == 0) | (ctx == last)
    is_helper = (ctx == 1) | (ctx == last - 1)
    helped = jnp.where(ctx == 1, 0, last)
    other_group = lax.rem(group + 1, groups)
    pair = tp + 1 - 2 * lax.rem(tp, 2)
    across = lax.rem(tp + 2, n)
    pair_across = lax.rem(pair + 2, n)

    def remote(src, dst, send, recv, to_ctx, to_tp):
        return pltpu.make_async_remote_copy(
            src_ref=src, dst_ref=dst, send_sem=send, recv_sem=recv,
            device_id={"ctx": to_ctx, "tp": to_tp}, device_id_type=MESH,
        )

    barrier = pltpu.get_barrier_semaphore()

    def greet(**device):
        pl.semaphore_signal(barrier, inc=1, device_id=device, device_id_type=MESH)

    @pl.when(ctx > 0)
    def _():
        greet(ctx=ctx - 1)

    @pl.when(ctx < last)
    def _():
        greet(ctx=ctx + 1)

    @pl.when(ctx == back)
    def _():
        greet(ctx=ctx - back)

    for step in range(1, n):
        greet(tp=lax.rem(tp + step, n))

    @pl.when(is_helper)
    def _():
        greet(groups=other_group)

    greetings = n - 1 + sum(
        flag.astype(jnp.int32) for flag in (ctx > 0, ctx < last, ctx == 0, is_helper)
    )

    first_row = pl.multiple_of(ctx * rows, rows)
    loads = [
        pltpu.make_async_copy(key_ref, key_in, load_sem.at[0]),
        pltpu.make_async_copy(table_ref.at[:, pl.ds(first_row, rows)], table, load_sem.at[1]),
        pltpu.make_async_copy(doc_ref, docs, load_sem.at[2]),
        pltpu.make_async_copy(query_ref, query_in, load_sem.at[3]),
    ]
    value_loads = [
        pltpu.make_async_copy(
            value_ref.at[:, pl.ds(head * HEAD_SIZE, HEAD_SIZE)], kv.at[back, head, 1], load_sem.at[4 + head]
        )
        for head in range(kv_heads)
    ]
    lent_start = starts[lent_chunk] * HEAD_SIZE
    weight_rows = [pl.ds(lent_start, lent.shape[0]), pl.ds(0, lent_start)]
    weight_loads = [
        pltpu.make_async_copy(weight_ref.at[part], weight.at[part], weight_sem.at[index])
        for index, part in enumerate(weight_rows)
    ]
    for load in loads + value_loads + weight_loads:
        load.start()

    def turn(values):
        values = values.astype(jnp.float32)
        return (values * table[0] + pltpu.roll(values, HEAD_SIZE // 2, 1) * table[1]).astype(jnp.bfloat16)

    loads[0].wait()
    loads[1].wait()
    for head in range(kv_heads):
        kv[back, head, 0] = turn(key_in[:, head * HEAD_SIZE : (head + 1) * HEAD_SIZE])
    for load in value_loads:
        load.wait()

    for slot in range(back):
        @pl.when(ctx < back - slot)
        def _():
            kv[slot] = jnp.zeros(kv.shape[1:], kv.dtype)

    pl.semaphore_wait(barrier, greetings)

    def kv_copy(slot, head):
        return remote(
            kv.at[slot, head], kv.at[slot - 1, head], kv_send.at[slot, head], kv_recv.at[slot - 1, head],
            lax.rem(ctx + 1, n), tp,
        )

    def kv_direct(head):
        return remote(
            kv.at[back, head], kv.at[0, head], kv_send.at[0, head], kv_recv.at[0, head], lax.rem(ctx + back, n), tp
        )

    for head in range(kv_heads):
        @pl.when(ctx < last)
        def _():
            kv_copy(back, head).start()

        if head == 0:
            @pl.when(ctx == 0)
            def _():
                kv_direct(head).start()

    def lend_copy(piece):
        start = pl.multiple_of(group * half_rows + piece * piece_rows, piece_rows)
        return remote(
            weight.at[pl.ds(starts[lent_chunk] * HEAD_SIZE + start, piece_rows)], lent.at[pl.ds(start, piece_rows)],
            lend_send, lend_recv.at[piece], jnp.where(ctx == 0, 1, last - 1), tp,
        )

    def share_copy(piece, owner):
        start = pl.multiple_of(owner * half_rows + piece * piece_rows, piece_rows)
        here = lent.at[pl.ds(start, piece_rows)]
        return pltpu.make_async_remote_copy(
            src_ref=here, dst_ref=here, send_sem=share_send, recv_sem=share_recv,
            device_id={"groups": other_group}, device_id_type=MESH,
        )

    weight_loads[0].wait()

    @pl.when(is_edge)
    def _():
        for piece in range(pieces):
            lend_copy(piece).start()

    loads[2].wait()
    own_docs = jnp.broadcast_to(docs[pl.ds(ctx, 1), :], (rows, rows)).astype(jnp.float32).T
    row_index = lax.broadcasted_iota(jnp.int32, (rows, rows), 0)
    column_index = lax.broadcasted_iota(jnp.int32, (rows, rows), 1)
    for slot in range(back + 1):
        block = ctx - back + slot
        their_docs = docs[pl.ds(lax.max(block, 0), 1), :].astype(jnp.float32)
        allowed = (own_docs == their_docs) & (block * rows + column_index <= ctx * rows + row_index) & (block >= 0)
        bias[slot] = jnp.where(allowed, 0.0, -1e30)

    loads[3].wait()
    for head in range(query_heads):
        rotated[head] = turn(query_in[:, head * HEAD_SIZE : (head + 1) * HEAD_SIZE])


    def forwards(head):
        return (ctx >= (back if head == 0 else back - 1)) & (ctx < last)

    def take_kv(head):
        kv_copy(back, head).wait_recv()

        @pl.when(forwards(head))
        def _():
            kv_copy(back - 1, head).start()

    for head in range(kv_heads):
        @pl.when(ctx >= (1 if head == 0 else back))
        def _():
            take_kv(head)

    away = jnp.where(ctx < n // 2, 1, -1)

    def block_at(distance):
        return ctx + distance * away

    def chunk_copy(block, chunk, send, to_ctx):
        here = gathered.at[block, :, columns_of(chunk)]
        return remote(here, here, send, chunk_recv.at[block, chunk], to_ctx, tp)

    def away_copy(block, chunk):
        return chunk_copy(block, chunk, away_send.at[jnp.where(block == ctx, 0, 1)], ctx + away)

    def edge_copy(block, chunk):
        return chunk_copy(block, chunk, edge_send.at[(block - ctx) * away], helped)

    scale = HEAD_SIZE ** (-0.5) * math.log2(math.e)
    contract = (((1,), (1,)), ((), ()))
    for head in range(query_heads):
        kv_head = head // group_width
        if head == ends[1] - 1:
            @pl.when((ctx >= 1) & (ctx < back))
            def _():
                for other in range(1, kv_heads):
                    take_kv(other)

        if head % group_width == 0:
            @pl.when(ctx >= back)
            def _():
                kv_copy(1, kv_head).wait_recv()

        scores = [
            lax.dot_general(rotated[head], kv[slot, kv_head, 0], contract, preferred_element_type=jnp.float32) * scale
            + bias[slot]
            for slot in range(back + 1)
        ]
        row_max = functools.reduce(jnp.maximum, scores).max(-1, keepdims=True)
        weights = [jnp.exp2(score - row_max) for score in scores]
        totals = sum(weights).sum(-1, keepdims=True)
        mixed = sum(
            jnp.dot(weights[slot].astype(jnp.bfloat16), kv[slot, kv_head, 1], preferred_element_type=jnp.float32)
            for slot in range(back + 1)
        )
        gathered[ctx, :, head * HEAD_SIZE : (head + 1) * HEAD_SIZE] = (mixed / totals).astype(jnp.bfloat16)
        if head + 1 in ends:
            chunk = ends.index(head + 1)
            away_copy(ctx, chunk).start()
            if chunk != lent_chunk:
                @pl.when(is_helper)
                def _():
                    edge_copy(ctx, chunk).start()

    def pass_on(piece):
        lend_copy(piece).wait_recv()
        share_copy(piece, group).start()

    @pl.when(is_helper)
    def _():
        pass_on(0)
        pass_on(1)

    def pair_copy(place, index):
        return remote(
            partial.at[place, pair_across if index else pair], pair_in.at[place, index],
            pair_send, pair_recv.at[place, index], ctx, pair,
        )

    def cross_copy(place):
        return remote(
            crossing.at[place], cross_in.at[place], cross_send, cross_recv.at[place], ctx, across
        )

    parts = (pair_across, pair, across, tp)

    def part_columns(part):
        return pl.ds(pl.multiple_of(part * quarter, quarter), quarter)

    def emit(place, index, product):
        partial[place, parts[index]] = product.astype(jnp.bfloat16)
        if index < 2:
            pair_copy(place, 1 - index).start()

    def project(block, chunk, keep, final):
        for index, part in enumerate(parts):
            product = jnp.dot(
                gathered[block, :, columns_of(chunk)], weight[columns_of(chunk), part_columns(part)],
                preferred_element_type=jnp.float32,
            )
            if chunk > 0:
                product = product + sums[keep, index]
            if chunk == final:
                emit(block, index, product)
            else:
                sums[keep, index] = product

    def cross(place):
        pair_copy(place, 1).wait_recv()
        value = partial[place, across].astype(jnp.float32) + pair_in[place, 1].astype(jnp.float32)
        crossing[place] = value.astype(jnp.bfloat16)
        cross_copy(place).start()

    def collect(place):
        pair_copy(place, 0).wait_recv()
        value = partial[place, tp].astype(jnp.float32) + pair_in[place, 0].astype(jnp.float32)
        cross_copy(place).wait_recv()
        return (value + cross_in[place].astype(jnp.float32)).astype(jnp.bfloat16)

    def result_copy(block):
        return remote(
            summed.at[block], landed.at[tp], result_send, result_recv, block, ctx
        )

    def finish(block):
        value = collect(block)
        mine = (block == ctx) & (tp == ctx)

        @pl.when(mine)
        def _():
            landed[tp] = value

        @pl.when(jnp.logical_not(mine))
        def _():
            summed[block] = value
            result_copy(block).start()

    for load in weight_loads[1:]:
        load.wait()
    for chunk in range(chunks):
        project(ctx, chunk, 0, lent_chunk)

    def aid_copy(index):
        return remote(
            summed.at[n + index], landed_aid.at[tp], result_send, aid_recv,
            block_at(index), helped,
        )

    far_block = jnp.where(ctx < n // 2, last, 0)
    sends_far = ctx != 1

    def far_copy(index):
        return remote(
            halves.at[index], landed_far.at[tp, index], half_send, far_recv, far_block, ctx
        )

    def pair_sum(place, index):
        pair_copy(place, index).wait_recv()
        part = across if index else tp
        value = partial[place, part].astype(jnp.float32) + pair_in[place, index].astype(jnp.float32)
        return value.astype(jnp.bfloat16)

    def finish_far():
        for index in (1, 0):
            halves[index] = pair_sum(far_block, index)
            far_copy(index).start()

    def aid(index):
        for position, part in enumerate(parts):
            product = jnp.dot(
                gathered[block_at(index), :, columns_of(lent_chunk)], lent[:, part_columns(part)],
                preferred_element_type=jnp.float32,
            )
            emit(n + index, position, product)

    def finish_aid(index):
        value = collect(n + index)
        if index == 0:
            @pl.when(tp == helped)
            def _():
                landed_aid[tp] = value

            @pl.when(tp != helped)
            def _():
                summed[n] = value
                aid_copy(0).start()
        else:
            summed[n + index] = value
            aid_copy(index).start()

    def take(block, chunk, forward):
        away_copy(block, chunk).wait_recv()
        if forward is not None:
            forward(block, chunk).start()

    @pl.when(is_edge)
    def _():
        def gather_step(distance, carry):
            block = block_at(distance)
            for chunk in range(lent_chunk):
                if chunk == lent_chunk - 1:
                    finish(block_at(distance - 1))
                take(block, chunk, None)
                project(block, chunk, 1, lent_chunk - 1)
                if chunk == 0:
                    cross(block_at(distance - 1))
            return carry

        lax.fori_loop(1, n, gather_step, 0)
        finish_far()

    def near(chunk):
        take(helped, chunk, away_copy)
        project(helped, chunk, 0, lent_chunk)

    def far(distance, chunk):
        take(block_at(distance), chunk, edge_copy if chunk < lent_chunk else None)
        project(block_at(distance), chunk, distance, lent_chunk)

    def aid_both():
        arrived = lent.at[pl.ds(pl.multiple_of(other_group * half_rows, half_rows), half_rows)]
        remote(arrived, arrived, share_send, share_recv, ctx, pair).wait_recv()
        aid(1)
        aid(0)

    def last_chunks():
        far(2, lent_chunk)
        aid(2)
        cross(n + 2)

    @pl.when(ctx == 1)
    def _():
        far(1, 0)
        pass_on(2)
        far(1, 1)
        pass_on(3)
        cross(ctx)
        near(0)
        far(1, 2)
        far(1, 3)
        near(1)
        finish(ctx)
        far(1, lent_chunk)
        near(2)
        cross(block_at(1))
        far(2, 0)
        aid_both()
        near(3)
        far(2, 1)
        cross(n + 1)
        cross(n)
        near(lent_chunk)
        far(2, 2)
        finish(block_at(1))
        cross(helped)
        far(2, 3)
        finish_aid(1)
        last_chunks()
        cross(far_block)
        finish_aid(0)
        finish(helped)
        finish_aid(2)
        finish(far_block)

    @pl.when(ctx == last - 1)
    def _():
        pass_on(2)
        far(1, 0)
        pass_on(3)
        near(0)
        far(1, 1)
        cross(ctx)
        near(1)
        far(1, 2)
        far(1, 3)
        near(2)
        far(1, lent_chunk)
        finish(ctx)
        near(3)
        cross(block_at(1))
        near(lent_chunk)
        aid_both()
        far(2, 0)
        cross(helped)
        cross(n + 1)
        cross(n)
        far(2, 1)
        far(2, 2)
        finish(block_at(1))
        finish(helped)
        far(2, 3)
        finish_aid(1)
        last_chunks()
        finish_far()
        finish_aid(0)
        finish_aid(2)

    is_far = ((ctx == 0) & (tp >= n // 2)) | ((ctx == last) & (tp == 0))
    gets_aid = ((tp == 0) | (tp == last)) & (ctx != tp)
    aid_here = is_helper & (tp == helped)

    def landed_all(landing, recv, local):
        if local is None:
            return remote(landing, landing, half_send, recv, ctx, pair).wait_recv()

        @pl.when(local)
        def _():
            some = landing.at[pl.ds(0, n - 1)]
            remote(some, some, half_send, recv, ctx, pair).wait_recv()

        @pl.when(jnp.logical_not(local))
        def _():
            remote(landing, landing, half_send, recv, ctx, pair).wait_recv()

    @pl.when(is_far)
    def _():
        landed_all(landed_far, far_recv, None)

    @pl.when(jnp.logical_not(is_far))
    def _():
        landed_all(landed, result_recv, tp == ctx)

    @pl.when(gets_aid)
    def _():
        landed_all(landed_aid, aid_recv, aid_here)

    def both_halves(landing, part):
        return landing[part, 0].astype(jnp.float32) + landing[(part + 2) % n, 1].astype(jnp.float32)

    for part in range(n):
        columns = pl.ds(part * quarter, quarter)

        @pl.when(is_far & jnp.logical_not(gets_aid))
        def _():
            out_ref[:, columns] = both_halves(landed_far, part).astype(jnp.bfloat16)

        @pl.when(is_far & gets_aid)
        def _():
            whole = both_halves(landed_far, part) + landed_aid[part].astype(jnp.float32)
            out_ref[:, columns] = whole.astype(jnp.bfloat16)

        @pl.when(gets_aid & jnp.logical_not(is_far))
        def _():
            whole = landed[part].astype(jnp.float32) + landed_aid[part].astype(jnp.float32)
            out_ref[:, columns] = whole.astype(jnp.bfloat16)

        @pl.when(jnp.logical_not(gets_aid | is_far))
        def _():
            out_ref[:, columns] = landed[part]

    for head in range(kv_heads):
        @pl.when(ctx < last)
        def _():
            kv_copy(back, head).wait_send()

        if head == 0:
            @pl.when(ctx == 0)
            def _():
                kv_direct(head).wait_send()

        @pl.when(forwards(head))
        def _():
            kv_copy(back - 1, head).wait_send()

    def sent(source, send):
        remote(source, source, send, chunk_recv.at[0, 0], ctx, pair).wait_send()

    half_lent = lent.at[pl.ds(0, half_rows)]
    sent(gathered.at[ctx], away_send.at[0])

    @pl.when(is_edge)
    def _():
        sent(half_lent, lend_send)
        sent(pair_in.at[pl.ds(0, n)], pair_send)
        sent(cross_in.at[pl.ds(0, n - 1)], cross_send)

    @pl.when(is_helper)
    def _():
        sent(half_lent, share_send)
        sent(gathered.at[helped], away_send.at[1])
        sent(pair_in, pair_send)
        for distance in range(n - 1):
            sent(gathered.at[block_at(distance), :, pl.ds(0, starts[lent_chunk] * HEAD_SIZE)], edge_send.at[distance])

    @pl.when(ctx == 1)
    def _():
        sent(cross_in, cross_send)

    @pl.when(ctx == last - 1)
    def _():
        sent(cross_in.at[pl.ds(0, 2 * n - 2)], cross_send)

    def sent_results(count):
        local = (tp == ctx) | (is_helper & (tp == helped))

        @pl.when(local)
        def _():
            sent(summed.at[pl.ds(0, count - 1)], result_send)

        @pl.when(jnp.logical_not(local))
        def _():
            sent(summed.at[pl.ds(0, count)], result_send)

    @pl.when(is_edge)
    def _():
        sent_results(n - 1)

    @pl.when(ctx == 1)
    def _():
        sent_results(2 * n - 1)

    @pl.when(ctx == last - 1)
    def _():
        sent_results(2 * n - 2)

    @pl.when(sends_far)
    def _():
        sent(halves, half_send)


def chunk_ends(heads, groups):
    lent = max(1, round(heads * LENT_SHARE))
    kept = heads - lent
    return [heads // 8, heads * 3 // 8, heads * 5 // 8, kept, heads]


def key_blocks_back(tokens, rows):
    return -(-(tokens // 2 - 1) // rows)


def fused(n, groups, query_matrix, key_matrix, value_matrix, doc_ids, out_weight):
    rows, query_width = query_matrix.shape
    query_heads, kv_heads = query_width // HEAD_SIZE, key_matrix.shape[1] // HEAD_SIZE
    features = out_weight.shape[1]
    tokens = doc_ids.shape[0]
    back = key_blocks_back(tokens, rows)
    chunks = len(chunk_ends(query_heads, groups))
    lent_rows = query_width - chunk_ends(query_heads, groups)[-2] * HEAD_SIZE
    pieces = 4
    quarter = features // n
    half = HEAD_SIZE // 2
    frequency = np.power(np.float32(rope_base), -np.arange(half, dtype=np.float32) * np.float32(2.0 / HEAD_SIZE))
    angles = np.arange(tokens, dtype=np.float32)[:, None] * frequency[None, :]
    cosine, sine = np.cos(angles), np.sin(angles)
    table = np.stack([np.concatenate([cosine, cosine], 1), np.concatenate([-sine, sine], 1)]).astype(np.float32)
    any_space = pl.BlockSpec(memory_space=pl.ANY)
    bf16, f32, dma = jnp.bfloat16, jnp.float32, pltpu.SemaphoreType.DMA
    return pl.pallas_call(
        functools.partial(fused_kernel, n, groups, back),
        out_shape=pltpu.VMEM((rows, features), bf16),
        in_specs=[any_space] * 6,
        out_specs=pl.BlockSpec(memory_space=pltpu.VMEM),
        scratch_shapes=[
            pltpu.VMEM((rows, query_width), bf16),
            pltpu.VMEM((rows, kv_heads * HEAD_SIZE), bf16),
            pltpu.VMEM((2, rows, HEAD_SIZE), f32),
            pltpu.VMEM((tokens // rows, rows), jnp.int32),
            pltpu.VMEM((query_width, features), bf16),
            pltpu.VMEM((lent_rows, features), bf16),
            pltpu.VMEM((query_heads, rows, HEAD_SIZE), bf16),
            pltpu.VMEM((back + 1, rows, rows), f32),
            pltpu.VMEM((back + 1, kv_heads, 2, rows, HEAD_SIZE), bf16),
            pltpu.VMEM((n, rows, query_width), bf16),
            pltpu.VMEM((3, n, rows, quarter), f32),
            pltpu.VMEM((2 * n - 1, n, rows, quarter), bf16),
            pltpu.VMEM((2 * n - 1, 2, rows, quarter), bf16),
            pltpu.VMEM((2 * n - 1, rows, quarter), bf16),
            pltpu.VMEM((2 * n - 1, rows, quarter), bf16),
            pltpu.VMEM((2 * n - 1, rows, quarter), bf16),
            pltpu.VMEM((n, rows, quarter), bf16),
            pltpu.VMEM((2, rows, quarter), bf16),
            pltpu.VMEM((n, 2, rows, quarter), bf16),
            pltpu.VMEM((n, rows, quarter), bf16),
            dma((4 + kv_heads,)),
            dma((2,)),
            dma((back + 1, kv_heads)),
            dma((back, kv_heads)),
            dma((2,)),
            dma((n - 1,)),
            dma((n, chunks)),
            dma,
            dma((pieces,)),
            dma,
            dma,
            dma,
            dma((2 * n - 1, 2)),
            dma,
            dma((2 * n - 1,)),
            dma,
            dma,
            dma,
            dma,
            dma,
        ],
        compiler_params=pltpu.CompilerParams(collective_id=0, has_side_effects=True),
    )(query_matrix, key_matrix, value_matrix, doc_ids.reshape(tokens // rows, rows), jnp.asarray(table), out_weight)


def solution(mesh):
    in_specs = (
        P(("groups", "ctx"), "tp"),
        P(("groups", "ctx"), "tp"),
        P(("groups", "ctx"), "tp"),
        P("groups"),
        P("tp", "ctx"),
    )
    out_specs = P(("groups", "ctx"), "tp")
    n, groups = mesh.shape["ctx"], mesh.shape["groups"]

    def body(*arrays):
        query_matrix, doc_ids = arrays[0], arrays[3]
        back = key_blocks_back(doc_ids.shape[0], query_matrix.shape[0])
        if n == mesh.shape["tp"] and n == 4 and groups == 2 and back == 2:
            return fused(n, groups, *arrays)
        return on_device(*arrays)

    return jax.shard_map(
        body, mesh=mesh, in_specs=in_specs, out_specs=out_specs, check_vma=False
    )
```

```python
import functools
import math

import jax
import jax.numpy as jnp
import numpy as np
from jax import lax
from jax.experimental import pallas as pl
from jax.experimental.pallas import tpu as pltpu
from jax.sharding import PartitionSpec as P

MESH = pl.DeviceIdType.MESH

HEAD_SIZE = 128


rope_base = 1000000.0

LENT_SHARE = 3 / 16


def rotary_tables(rows, token_positions, heads):
    half_dim = HEAD_SIZE // 2
    frequency = jnp.power(
        jnp.float32(rope_base), -jnp.arange(half_dim, dtype=jnp.float32) * (2.0 / HEAD_SIZE)
    )
    angles = token_positions.astype(jnp.float32)[:, None] * frequency[None, :]
    cosine = jnp.cos(angles)[:, None, :]
    sine = jnp.sin(angles)[:, None, :]
    values = rows.astype(jnp.float32).reshape(rows.shape[0], heads, HEAD_SIZE)
    first = values[..., :half_dim]
    second = values[..., half_dim:]
    turned = jnp.concatenate([first * cosine - second * sine, second * cosine + first * sine], -1)
    return turned.reshape(rows.shape[0], heads * HEAD_SIZE).astype(jnp.bfloat16)


def on_device(query_matrix, key_matrix, value_matrix, doc_ids, out_weight):
    ctx_index = lax.axis_index("ctx")
    tok_rows = query_matrix.shape[0]
    query_heads = query_matrix.shape[1] // HEAD_SIZE
    key_heads = key_matrix.shape[1] // HEAD_SIZE
    group_width = query_heads // key_heads
    inverse_root = HEAD_SIZE ** (-0.5)
    local_rows = jnp.arange(tok_rows, dtype=jnp.int32)
    given_pos = ctx_index * tok_rows + local_rows
    query_matrix_rot = rotary_tables(query_matrix, given_pos, query_heads)
    keys_here = rotary_tables(key_matrix, given_pos, key_heads)
    query_doc = jnp.take(doc_ids, given_pos, axis=0)
    query_four = query_matrix_rot.reshape(tok_rows, key_heads, group_width, HEAD_SIZE)

    def attend(state, block):
        key_block, value_block, doc_block, pos_block = block
        row_max, totals, accum = state
        scores = (
            jnp.einsum("qkgd,skd->kgqs", query_four, key_block, preferred_element_type=jnp.float32)
            * inverse_root
        )
        allowed = (
            (query_doc[:, None] == doc_block[None, :]) & (pos_block[None, :] <= given_pos[:, None])
        )[None, None]
        new_max = jnp.maximum(row_max, jnp.max(jnp.where(allowed, scores, -1e30), -1))
        weights = jnp.where(allowed, jnp.exp(scores - new_max[..., None]), 0.0)
        factor = jnp.exp(row_max - new_max)
        totals = totals * factor + jnp.sum(weights, -1)
        accum = accum * jnp.transpose(factor, (2, 0, 1))[..., None] + jnp.einsum(
            "kgqs,skd->qkgd",
            weights.astype(jnp.bfloat16),
            value_block,
            preferred_element_type=jnp.float32,
        )
        return (new_max, totals, accum)

    start_state = (
        jnp.full((key_heads, group_width, tok_rows), -1e30, jnp.float32),
        jnp.zeros((key_heads, group_width, tok_rows), jnp.float32),
        jnp.zeros((tok_rows, key_heads, group_width, HEAD_SIZE), jnp.float32),
    )
    key_piece = lax.all_gather(keys_here, "ctx", axis=0, tiled=True)
    value_piece = lax.all_gather(value_matrix, "ctx", axis=0, tiled=True)
    count = key_piece.shape[0]
    block_rows = math.gcd(count, 512)
    block_count = count // block_rows
    positions = jnp.arange(count, dtype=jnp.int32)
    blocks = (
        key_piece.reshape(block_count, block_rows, key_heads, HEAD_SIZE),
        value_piece.reshape(block_count, block_rows, key_heads, HEAD_SIZE),
        jnp.take(doc_ids, positions, axis=0).reshape(block_count, block_rows),
        positions.reshape(block_count, block_rows),
    )

    def step_block(inner_state, block):
        return (attend(inner_state, block), None)

    final_state, unused_out = lax.scan(step_block, start_state, blocks)
    row_max, totals, accum = final_state
    attention = (
        (accum / jnp.transpose(totals, (2, 0, 1))[..., None])
        .reshape(tok_rows, query_heads * HEAD_SIZE)
        .astype(jnp.bfloat16)
    )
    terms = jnp.dot(
        attention,
        lax.all_gather(out_weight, "ctx", axis=1, tiled=True),
        preferred_element_type=jnp.float32,
    )
    return lax.psum_scatter(terms.astype(jnp.bfloat16), "tp", scatter_dimension=1, tiled=True)


def fused_kernel(
    n, groups, back, query_ref, key_ref, value_ref, doc_ref, table_ref, weight_ref, out_ref,
    query_in, key_in, table, docs, weight, lent, rotated, bias, kv, gathered, sums,
    partial, pair_in, crossing, cross_in, summed, landed, halves, landed_far, landed_aid,
    load_sem, weight_sem, kv_send, kv_recv, away_send, edge_send, chunk_recv, lend_send, lend_recv,
    share_send, share_recv, pair_send, pair_recv, cross_send, cross_recv, result_send, result_recv,
    half_send, far_recv, aid_recv,
):
    group = lax.axis_index("groups")
    ctx = lax.axis_index("ctx")
    tp = lax.axis_index("tp")
    rows = query_ref.shape[0]
    kv_heads = key_ref.shape[1] // HEAD_SIZE
    query_heads = query_ref.shape[1] // HEAD_SIZE
    group_width = query_heads // kv_heads
    ends = chunk_ends(query_heads, groups)
    starts = [0] + ends[:-1]
    chunks = len(ends)
    quarter = partial.shape[3]
    last = n - 1
    lent_chunk = chunks - 1
    pieces = lend_recv.shape[0]
    half_rows = lent.shape[0] // groups
    piece_rows = half_rows // pieces

    def columns_of(chunk):
        return pl.ds(starts[chunk] * HEAD_SIZE, (ends[chunk] - starts[chunk]) * HEAD_SIZE)

    is_edge = (ctx == 0) | (ctx == last)
    is_helper = (ctx == 1) | (ctx == last - 1)
    helped = jnp.where(ctx == 1, 0, last)
    other_group = lax.rem(group + 1, groups)
    pair = tp + 1 - 2 * lax.rem(tp, 2)
    across = lax.rem(tp + 2, n)
    pair_across = lax.rem(pair + 2, n)

    def remote(src, dst, send, recv, to_ctx, to_tp):
        return pltpu.make_async_remote_copy(
            src_ref=src, dst_ref=dst, send_sem=send, recv_sem=recv,
            device_id={"ctx": to_ctx, "tp": to_tp}, device_id_type=MESH,
        )

    barrier = pltpu.get_barrier_semaphore()

    def greet(**device):
        pl.semaphore_signal(barrier, inc=1, device_id=device, device_id_type=MESH)

    @pl.when(ctx > 0)
    def _():
        greet(ctx=ctx - 1)

    @pl.when(ctx < last)
    def _():
        greet(ctx=ctx + 1)

    @pl.when(ctx == back)
    def _():
        greet(ctx=ctx - back)

    for step in range(1, n):
        greet(tp=lax.rem(tp + step, n))

    @pl.when(is_helper)
    def _():
        greet(groups=other_group)

    greetings = n - 1 + sum(
        flag.astype(jnp.int32) for flag in (ctx > 0, ctx < last, ctx == 0, is_helper)
    )

    first_row = pl.multiple_of(ctx * rows, rows)
    loads = [
        pltpu.make_async_copy(key_ref, key_in, load_sem.at[0]),
        pltpu.make_async_copy(table_ref.at[:, pl.ds(first_row, rows)], table, load_sem.at[1]),
        pltpu.make_async_copy(doc_ref, docs, load_sem.at[2]),
        pltpu.make_async_copy(query_ref, query_in, load_sem.at[3]),
    ]
    value_loads = [
        pltpu.make_async_copy(
            value_ref.at[:, pl.ds(head * HEAD_SIZE, HEAD_SIZE)], kv.at[back, head, 1], load_sem.at[4 + head]
        )
        for head in range(kv_heads)
    ]
    lent_start = starts[lent_chunk] * HEAD_SIZE
    weight_rows = [pl.ds(lent_start, lent.shape[0]), pl.ds(0, lent_start)]
    weight_loads = [
        pltpu.make_async_copy(weight_ref.at[part], weight.at[part], weight_sem.at[index])
        for index, part in enumerate(weight_rows)
    ]
    for load in loads + value_loads + weight_loads:
        load.start()

    def turn(values):
        values = values.astype(jnp.float32)
        return (values * table[0] + pltpu.roll(values, HEAD_SIZE // 2, 1) * table[1]).astype(jnp.bfloat16)

    loads[0].wait()
    loads[1].wait()
    for head in range(kv_heads):
        kv[back, head, 0] = turn(key_in[:, head * HEAD_SIZE : (head + 1) * HEAD_SIZE])
    for load in value_loads:
        load.wait()

    for slot in range(back):
        @pl.when(ctx < back - slot)
        def _():
            kv[slot] = jnp.zeros(kv.shape[1:], kv.dtype)

    pl.semaphore_wait(barrier, greetings)

    def kv_copy(slot, head):
        return remote(
            kv.at[slot, head], kv.at[slot - 1, head], kv_send.at[slot, head], kv_recv.at[slot - 1, head],
            lax.rem(ctx + 1, n), tp,
        )

    def kv_direct(head):
        return remote(
            kv.at[back, head], kv.at[0, head], kv_send.at[0, head], kv_recv.at[0, head], lax.rem(ctx + back, n), tp
        )

    for head in range(kv_heads):
        @pl.when(ctx < last)
        def _():
            kv_copy(back, head).start()

        if head == 0:
            @pl.when(ctx == 0)
            def _():
                kv_direct(head).start()

    def lend_copy(piece):
        start = pl.multiple_of(group * half_rows + piece * piece_rows, piece_rows)
        return remote(
            weight.at[pl.ds(starts[lent_chunk] * HEAD_SIZE + start, piece_rows)], lent.at[pl.ds(start, piece_rows)],
            lend_send, lend_recv.at[piece], jnp.where(ctx == 0, 1, last - 1), tp,
        )

    def share_copy(piece, owner):
        start = pl.multiple_of(owner * half_rows + piece * piece_rows, piece_rows)
        here = lent.at[pl.ds(start, piece_rows)]
        return pltpu.make_async_remote_copy(
            src_ref=here, dst_ref=here, send_sem=share_send, recv_sem=share_recv,
            device_id={"groups": other_group}, device_id_type=MESH,
        )

    weight_loads[0].wait()

    @pl.when(is_edge)
    def _():
        for piece in range(pieces):
            lend_copy(piece).start()

    loads[2].wait()
    own_docs = jnp.broadcast_to(docs[pl.ds(ctx, 1), :], (rows, rows)).astype(jnp.float32).T
    row_index = lax.broadcasted_iota(jnp.int32, (rows, rows), 0)
    column_index = lax.broadcasted_iota(jnp.int32, (rows, rows), 1)
    for slot in range(back + 1):
        block = ctx - back + slot
        their_docs = docs[pl.ds(lax.max(block, 0), 1), :].astype(jnp.float32)
        allowed = (own_docs == their_docs) & (block * rows + column_index <= ctx * rows + row_index) & (block >= 0)
        bias[slot] = jnp.where(allowed, 0.0, -1e30)

    loads[3].wait()
    for head in range(query_heads):
        rotated[head] = turn(query_in[:, head * HEAD_SIZE : (head + 1) * HEAD_SIZE])


    def forwards(head):
        return (ctx >= (back if head == 0 else back - 1)) & (ctx < last)

    def take_kv(head):
        kv_copy(back, head).wait_recv()

        @pl.when(forwards(head))
        def _():
            kv_copy(back - 1, head).start()

    for head in range(kv_heads):
        @pl.when(ctx >= (1 if head == 0 else back))
        def _():
            take_kv(head)

    away = jnp.where(ctx < n // 2, 1, -1)

    def block_at(distance):
        return ctx + distance * away

    def chunk_copy(block, chunk, send, to_ctx):
        here = gathered.at[block, :, columns_of(chunk)]
        return remote(here, here, send, chunk_recv.at[block, chunk], to_ctx, tp)

    def away_copy(block, chunk):
        return chunk_copy(block, chunk, away_send.at[jnp.where(block == ctx, 0, 1)], ctx + away)

    def edge_copy(block, chunk):
        return chunk_copy(block, chunk, edge_send.at[(block - ctx) * away], helped)

    scale = HEAD_SIZE ** (-0.5) * math.log2(math.e)
    contract = (((1,), (1,)), ((), ()))
    for head in range(query_heads):
        kv_head = head // group_width
        if head == ends[1] - 1:
            @pl.when((ctx >= 1) & (ctx < back))
            def _():
                for other in range(1, kv_heads):
                    take_kv(other)

        if head % group_width == 0:
            @pl.when(ctx >= back)
            def _():
                kv_copy(1, kv_head).wait_recv()

        scores = [
            lax.dot_general(rotated[head], kv[slot, kv_head, 0], contract, preferred_element_type=jnp.float32) * scale
            + bias[slot]
            for slot in range(back + 1)
        ]
        row_max = functools.reduce(jnp.maximum, scores).max(-1, keepdims=True)
        weights = [jnp.exp2(score - row_max) for score in scores]
        totals = sum(weights).sum(-1, keepdims=True)
        mixed = sum(
            jnp.dot(weights[slot].astype(jnp.bfloat16), kv[slot, kv_head, 1], preferred_element_type=jnp.float32)
            for slot in range(back + 1)
        )
        gathered[ctx, :, head * HEAD_SIZE : (head + 1) * HEAD_SIZE] = (mixed / totals).astype(jnp.bfloat16)
        if head + 1 in ends:
            chunk = ends.index(head + 1)
            away_copy(ctx, chunk).start()
            if chunk != lent_chunk:
                @pl.when(is_helper)
                def _():
                    edge_copy(ctx, chunk).start()

    def pass_on(piece):
        lend_copy(piece).wait_recv()
        share_copy(piece, group).start()

    @pl.when(is_helper)
    def _():
        pass_on(0)
        pass_on(1)

    def pair_copy(place, index):
        return remote(
            partial.at[place, pair_across if index else pair], pair_in.at[place, index],
            pair_send, pair_recv.at[place, index], ctx, pair,
        )

    def cross_copy(place):
        return remote(
            crossing.at[place], cross_in.at[place], cross_send, cross_recv.at[place], ctx, across
        )

    parts = (pair_across, pair, across, tp)

    def part_columns(part):
        return pl.ds(pl.multiple_of(part * quarter, quarter), quarter)

    def emit(place, index, product):
        partial[place, parts[index]] = product.astype(jnp.bfloat16)
        if index < 2:
            pair_copy(place, 1 - index).start()

    def project(block, chunk, keep, final):
        for index, part in enumerate(parts):
            product = jnp.dot(
                gathered[block, :, columns_of(chunk)], weight[columns_of(chunk), part_columns(part)],
                preferred_element_type=jnp.float32,
            )
            if chunk > 0:
                product = product + sums[keep, index]
            if chunk == final:
                emit(block, index, product)
            else:
                sums[keep, index] = product

    def cross(place):
        pair_copy(place, 1).wait_recv()
        value = partial[place, across].astype(jnp.float32) + pair_in[place, 1].astype(jnp.float32)
        crossing[place] = value.astype(jnp.bfloat16)
        cross_copy(place).start()

    def collect(place):
        pair_copy(place, 0).wait_recv()
        value = partial[place, tp].astype(jnp.float32) + pair_in[place, 0].astype(jnp.float32)
        cross_copy(place).wait_recv()
        return (value + cross_in[place].astype(jnp.float32)).astype(jnp.bfloat16)

    def result_copy(block):
        return remote(
            summed.at[block], landed.at[tp], result_send, result_recv, block, ctx
        )

    def finish(block):
        value = collect(block)
        mine = (block == ctx) & (tp == ctx)

        @pl.when(mine)
        def _():
            landed[tp] = value

        @pl.when(jnp.logical_not(mine))
        def _():
            summed[block] = value
            result_copy(block).start()

    for load in weight_loads[1:]:
        load.wait()
    for chunk in range(chunks):
        project(ctx, chunk, 0, lent_chunk)

    def aid_copy(index):
        return remote(
            summed.at[n + index], landed_aid.at[tp], result_send, aid_recv,
            block_at(index), helped,
        )

    far_block = jnp.where(ctx < n // 2, last, 0)
    sends_far = ctx != 1

    def far_copy(index):
        return remote(
            halves.at[index], landed_far.at[tp, index], half_send, far_recv, far_block, ctx
        )

    def pair_sum(place, index):
        pair_copy(place, index).wait_recv()
        part = across if index else tp
        value = partial[place, part].astype(jnp.float32) + pair_in[place, index].astype(jnp.float32)
        return value.astype(jnp.bfloat16)

    def finish_far():
        for index in (1, 0):
            halves[index] = pair_sum(far_block, index)
            far_copy(index).start()

    def aid(index):
        for position, part in enumerate(parts):
            product = jnp.dot(
                gathered[block_at(index), :, columns_of(lent_chunk)], lent[:, part_columns(part)],
                preferred_element_type=jnp.float32,
            )
            emit(n + index, position, product)

    def finish_aid(index):
        value = collect(n + index)
        if index == 0:
            @pl.when(tp == helped)
            def _():
                landed_aid[tp] = value

            @pl.when(tp != helped)
            def _():
                summed[n] = value
                aid_copy(0).start()
        else:
            summed[n + index] = value
            aid_copy(index).start()

    def take(block, chunk, forward):
        away_copy(block, chunk).wait_recv()
        if forward is not None:
            forward(block, chunk).start()

    @pl.when(is_edge)
    def _():
        def gather_step(distance, carry):
            block = block_at(distance)
            for chunk in range(lent_chunk):
                if chunk == lent_chunk - 1:
                    finish(block_at(distance - 1))
                take(block, chunk, None)
                project(block, chunk, 1, lent_chunk - 1)
                if chunk == 0:
                    cross(block_at(distance - 1))
            return carry

        lax.fori_loop(1, n, gather_step, 0)
        finish_far()

    def near(chunk):
        take(helped, chunk, away_copy)
        project(helped, chunk, 0, lent_chunk)

    def far(distance, chunk):
        take(block_at(distance), chunk, edge_copy if chunk < lent_chunk else None)
        project(block_at(distance), chunk, distance, lent_chunk)

    def aid_both():
        arrived = lent.at[pl.ds(pl.multiple_of(other_group * half_rows, half_rows), half_rows)]
        remote(arrived, arrived, share_send, share_recv, ctx, pair).wait_recv()
        aid(1)
        aid(0)

    def last_chunks():
        far(2, lent_chunk)
        aid(2)
        cross(n + 2)

    @pl.when(ctx == 1)
    def _():
        far(1, 0)
        pass_on(2)
        far(1, 1)
        pass_on(3)
        cross(ctx)
        near(0)
        far(1, 2)
        far(1, 3)
        near(1)
        finish(ctx)
        far(1, lent_chunk)
        near(2)
        cross(block_at(1))
        far(2, 0)
        aid_both()
        near(3)
        far(2, 1)
        cross(n + 1)
        cross(n)
        near(lent_chunk)
        far(2, 2)
        finish(block_at(1))
        cross(helped)
        far(2, 3)
        finish_aid(1)
        last_chunks()
        cross(far_block)
        finish_aid(0)
        finish(helped)
        finish_aid(2)
        finish(far_block)

    @pl.when(ctx == last - 1)
    def _():
        pass_on(2)
        far(1, 0)
        pass_on(3)
        near(0)
        far(1, 1)
        cross(ctx)
        near(1)
        far(1, 2)
        far(1, 3)
        near(2)
        far(1, lent_chunk)
        finish(ctx)
        near(3)
        cross(block_at(1))
        near(lent_chunk)
        aid_both()
        far(2, 0)
        cross(helped)
        cross(n + 1)
        cross(n)
        far(2, 1)
        far(2, 2)
        finish(block_at(1))
        finish(helped)
        far(2, 3)
        finish_aid(1)
        last_chunks()
        finish_far()
        finish_aid(0)
        finish_aid(2)

    is_far = ((ctx == 0) & (tp >= n // 2)) | ((ctx == last) & (tp == 0))
    gets_aid = ((tp == 0) | (tp == last)) & (ctx != tp)
    aid_here = is_helper & (tp == helped)

    def landed_all(landing, recv, local):
        if local is None:
            return remote(landing, landing, half_send, recv, ctx, pair).wait_recv()

        @pl.when(local)
        def _():
            some = landing.at[pl.ds(0, n - 1)]
            remote(some, some, half_send, recv, ctx, pair).wait_recv()

        @pl.when(jnp.logical_not(local))
        def _():
            remote(landing, landing, half_send, recv, ctx, pair).wait_recv()

    @pl.when(is_far)
    def _():
        landed_all(landed_far, far_recv, None)

    @pl.when(jnp.logical_not(is_far))
    def _():
        landed_all(landed, result_recv, tp == ctx)

    @pl.when(gets_aid)
    def _():
        landed_all(landed_aid, aid_recv, aid_here)

    def both_halves(landing, part):
        return landing[part, 0].astype(jnp.float32) + landing[(part + 2) % n, 1].astype(jnp.float32)

    for part in range(n):
        columns = pl.ds(part * quarter, quarter)

        @pl.when(is_far & jnp.logical_not(gets_aid))
        def _():
            out_ref[:, columns] = both_halves(landed_far, part).astype(jnp.bfloat16)

        @pl.when(is_far & gets_aid)
        def _():
            whole = both_halves(landed_far, part) + landed_aid[part].astype(jnp.float32)
            out_ref[:, columns] = whole.astype(jnp.bfloat16)

        @pl.when(gets_aid & jnp.logical_not(is_far))
        def _():
            whole = landed[part].astype(jnp.float32) + landed_aid[part].astype(jnp.float32)
            out_ref[:, columns] = whole.astype(jnp.bfloat16)

        @pl.when(jnp.logical_not(gets_aid | is_far))
        def _():
            out_ref[:, columns] = landed[part]

    for head in range(kv_heads):
        @pl.when(ctx < last)
        def _():
            kv_copy(back, head).wait_send()

        if head == 0:
            @pl.when(ctx == 0)
            def _():
                kv_direct(head).wait_send()

        @pl.when(forwards(head))
        def _():
            kv_copy(back - 1, head).wait_send()

    def sent(source, send):
        remote(source, source, send, chunk_recv.at[0, 0], ctx, pair).wait_send()

    half_lent = lent.at[pl.ds(0, half_rows)]
    sent(gathered.at[ctx], away_send.at[0])

    @pl.when(is_edge)
    def _():
        sent(half_lent, lend_send)
        sent(pair_in.at[pl.ds(0, n)], pair_send)
        sent(cross_in.at[pl.ds(0, n - 1)], cross_send)

    @pl.when(is_helper)
    def _():
        sent(half_lent, share_send)
        sent(gathered.at[helped], away_send.at[1])
        sent(pair_in, pair_send)
        for distance in range(n - 1):
            sent(gathered.at[block_at(distance), :, pl.ds(0, starts[lent_chunk] * HEAD_SIZE)], edge_send.at[distance])

    @pl.when(ctx == 1)
    def _():
        sent(cross_in, cross_send)

    @pl.when(ctx == last - 1)
    def _():
        sent(cross_in.at[pl.ds(0, 2 * n - 2)], cross_send)

    def sent_results(count):
        local = (tp == ctx) | (is_helper & (tp == helped))

        @pl.when(local)
        def _():
            sent(summed.at[pl.ds(0, count - 1)], result_send)

        @pl.when(jnp.logical_not(local))
        def _():
            sent(summed.at[pl.ds(0, count)], result_send)

    @pl.when(is_edge)
    def _():
        sent_results(n - 1)

    @pl.when(ctx == 1)
    def _():
        sent_results(2 * n - 1)

    @pl.when(ctx == last - 1)
    def _():
        sent_results(2 * n - 2)

    @pl.when(sends_far)
    def _():
        sent(halves, half_send)


def chunk_ends(heads, groups):
    lent = max(1, round(heads * LENT_SHARE))
    kept = heads - lent
    return [heads * 3 // 16, heads * 7 // 16, heads * 11 // 16, kept, heads]


def key_blocks_back(tokens, rows):
    return -(-(tokens // 2 - 1) // rows)


def fused(n, groups, query_matrix, key_matrix, value_matrix, doc_ids, out_weight):
    rows, query_width = query_matrix.shape
    query_heads, kv_heads = query_width // HEAD_SIZE, key_matrix.shape[1] // HEAD_SIZE
    features = out_weight.shape[1]
    tokens = doc_ids.shape[0]
    back = key_blocks_back(tokens, rows)
    chunks = len(chunk_ends(query_heads, groups))
    lent_rows = query_width - chunk_ends(query_heads, groups)[-2] * HEAD_SIZE
    pieces = 4
    quarter = features // n
    half = HEAD_SIZE // 2
    frequency = np.power(np.float32(rope_base), -np.arange(half, dtype=np.float32) * np.float32(2.0 / HEAD_SIZE))
    angles = np.arange(tokens, dtype=np.float32)[:, None] * frequency[None, :]
    cosine, sine = np.cos(angles), np.sin(angles)
    table = np.stack([np.concatenate([cosine, cosine], 1), np.concatenate([-sine, sine], 1)]).astype(np.float32)
    any_space = pl.BlockSpec(memory_space=pl.ANY)
    bf16, f32, dma = jnp.bfloat16, jnp.float32, pltpu.SemaphoreType.DMA
    return pl.pallas_call(
        functools.partial(fused_kernel, n, groups, back),
        out_shape=pltpu.VMEM((rows, features), bf16),
        in_specs=[any_space] * 6,
        out_specs=pl.BlockSpec(memory_space=pltpu.VMEM),
        scratch_shapes=[
            pltpu.VMEM((rows, query_width), bf16),
            pltpu.VMEM((rows, kv_heads * HEAD_SIZE), bf16),
            pltpu.VMEM((2, rows, HEAD_SIZE), f32),
            pltpu.VMEM((tokens // rows, rows), jnp.int32),
            pltpu.VMEM((query_width, features), bf16),
            pltpu.VMEM((lent_rows, features), bf16),
            pltpu.VMEM((query_heads, rows, HEAD_SIZE), bf16),
            pltpu.VMEM((back + 1, rows, rows), f32),
            pltpu.VMEM((back + 1, kv_heads, 2, rows, HEAD_SIZE), bf16),
            pltpu.VMEM((n, rows, query_width), bf16),
            pltpu.VMEM((3, n, rows, quarter), f32),
            pltpu.VMEM((2 * n - 1, n, rows, quarter), bf16),
            pltpu.VMEM((2 * n - 1, 2, rows, quarter), bf16),
            pltpu.VMEM((2 * n - 1, rows, quarter), bf16),
            pltpu.VMEM((2 * n - 1, rows, quarter), bf16),
            pltpu.VMEM((2 * n - 1, rows, quarter), bf16),
            pltpu.VMEM((n, rows, quarter), bf16),
            pltpu.VMEM((2, rows, quarter), bf16),
            pltpu.VMEM((n, 2, rows, quarter), bf16),
            pltpu.VMEM((n, rows, quarter), bf16),
            dma((4 + kv_heads,)),
            dma((2,)),
            dma((back + 1, kv_heads)),
            dma((back, kv_heads)),
            dma((2,)),
            dma((n - 1,)),
            dma((n, chunks)),
            dma,
            dma((pieces,)),
            dma,
            dma,
            dma,
            dma((2 * n - 1, 2)),
            dma,
            dma((2 * n - 1,)),
            dma,
            dma,
            dma,
            dma,
            dma,
        ],
        compiler_params=pltpu.CompilerParams(collective_id=0, has_side_effects=True),
    )(query_matrix, key_matrix, value_matrix, doc_ids.reshape(tokens // rows, rows), jnp.asarray(table), out_weight)


def solution(mesh):
    in_specs = (
        P(("groups", "ctx"), "tp"),
        P(("groups", "ctx"), "tp"),
        P(("groups", "ctx"), "tp"),
        P("groups"),
        P("tp", "ctx"),
    )
    out_specs = P(("groups", "ctx"), "tp")
    n, groups = mesh.shape["ctx"], mesh.shape["groups"]

    def body(*arrays):
        query_matrix, doc_ids = arrays[0], arrays[3]
        back = key_blocks_back(doc_ids.shape[0], query_matrix.shape[0])
        if n == mesh.shape["tp"] and n == 4 and groups == 2 and back == 2:
            return fused(n, groups, *arrays)
        return on_device(*arrays)

    return jax.shard_map(
        body, mesh=mesh, in_specs=in_specs, out_specs=out_specs, check_vma=False
    )
```
